256 devices in a mesh: gx: 64 (over x, z_hi, y, core), gy: 4 (over z_lo).
Axes of the slice: x: 4, y: 4, z: 8 (z_hi: 2, z_lo: 4; z = z_hi * 4 + z_lo), core: 2. Of those that a mesh axis runs over, the one named last changes fastest.
Arguments:
- adjoint: float32 [9, 256, 128, 512], P(None, 'gx', 'gy'), may hold values from -6 to 6
- buoyancy: float32 [256, 128, 512], P('gx', 'gy'), may hold values from 0.5 to 2
- lame_lambda: float32 [256, 128, 512], P('gx', 'gy'), may hold values from 0.5 to 2
- shear_mu: float32 [256, 128, 512], P('gx', 'gy'), may hold values from 0.3 to 1.2
- packed: int32 [64, 64, 4, 12, 256], P('gx', None, 'gy'), may hold values from -2147483648 to 2147483646
- scales: float32 [64, 64, 4, 12], P('gx', None, 'gy'), may hold values from 0.005 to 0.05
- perm: int32 [64, 64], P('gx'), may hold values from 0 to 63, each once within a row
Outputs:
- adjoint_out: float32 [9, 256, 128, 512], P(None, 'gx', 'gy')
- gradients: float32 [2, 256, 128, 512], P(None, 'gx', 'gy')
The draws below stay inside these ranges and needn't reach their ends.
Inputs may be any that keep to these rules, and one draw needn't show every extreme that they name: Each row of perm names every number 0 to 63 once. The words of packed are stored inputs and may cross devices as they are, four signed bytes to a word; only values that a program computes travel in float32.
All inputs are finite; a program needn't handle non-finite values.
Results may differ from the reference program's by a relative error of at most 0.0003.
Values sent between devices are 32-bit elements; how exact they have to be, the bound alone decides.
A program may use at most 128 MiB of HBM per device.

```python
import math
import jax
import jax.numpy as jnp
from jax import lax

CX = 4
CY = 32
CZ = 512
STEPS = 2
COMP = 12
OWNERS = 64
SEGW = 256
NX = 256
NY = 128
NZ = 512
N_GY = 4


def place_ends(values, key, low, top_value):
    longest = values.shape.index(max(values.shape))
    spots = []
    for shift in (0, 1):
        where = [jax.random.randint(jax.random.fold_in(key, axis), (), 0, length) for axis, length in enumerate(values.shape)]
        where[longest] = (where[longest] + shift) % values.shape[longest]
        spots.append(tuple(where))
    return values.at[spots[0]].set(low).at[spots[1]].set(top_value)


def steps_of(stream_key, extent, cuts, low, top_value):
    loudness = 1.0
    for position, parts in cuts:
        draws = jax.random.uniform(jax.random.fold_in(jax.random.fold_in(stream_key, 6), position), (parts,), jnp.float32, low / len(cuts), top_value / len(cuts))
        loudness = loudness * jnp.repeat(jnp.exp(draws), extent[position] // parts).reshape((-1,) + (1,) * (len(extent) - 1 - position))
    return loudness


def normal_values(own_key, shape, spread, bound, cuts=(), kind=jnp.bfloat16):
    values = jax.random.normal(own_key, shape, jnp.float32) * spread
    if len(cuts) > 0:
        values = steps_of(own_key, shape, cuts, -0.22, 0.18) * values
    return jnp.clip(values, min=-bound, max=bound).astype(kind)


def setup_inputs(seed: int = 0) -> dict:
    keys = jax.random.split(jax.random.key(seed), 8)
    adjoint = normal_values(keys[0], (9, NX, NY, NZ), 1.0, 6.0, ((1, 64), (2, 4)), jnp.float32)
    buoyancy = jnp.clip(jnp.exp(math.log(2.0) - 1.3862944 * jax.random.uniform(keys[1], (NX, NY, NZ), jnp.float32) ** steps_of(keys[1], (NX, NY, NZ), ((0, 64), (1, 4)), -0.2, 0.2)), 0.5, 2.0)
    lame_lambda = jnp.clip(jnp.exp(math.log(2.0) - 1.3862944 * jax.random.uniform(keys[2], (NX, NY, NZ), jnp.float32) ** steps_of(keys[2], (NX, NY, NZ), ((0, 64), (1, 4)), -0.2, 0.2)), 0.5, 2.0)
    shear_mu = jnp.clip(jnp.exp(math.log(1.2) - 1.3862944 * jax.random.uniform(keys[3], (NX, NY, NZ), jnp.float32) ** steps_of(keys[3], (NX, NY, NZ), ((0, 64), (1, 4)), -0.2, 0.2)), 0.3, 1.2)
    packed = place_ends(jax.random.randint(keys[4], (OWNERS, OWNERS, N_GY, COMP, SEGW), -2147483648, 2147483647), jax.random.fold_in(keys[4], 1), -2147483648, 2147483646).astype(jnp.int32)
    scales = jnp.clip(jnp.exp(math.log(0.05) - 2.3025851 * jax.random.uniform(keys[5], (OWNERS, OWNERS, N_GY, COMP), jnp.float32) ** steps_of(keys[5], (OWNERS, OWNERS, N_GY, COMP), ((0, 64), (2, 4)), -0.2, 0.2)), 0.005, 0.05)
    perm = jax.vmap(lambda own: jax.random.permutation(own, OWNERS))(jax.random.split(keys[6], OWNERS)).reshape((OWNERS, OWNERS)).astype(jnp.int32)
    return dict(adjoint=adjoint, buoyancy=buoyancy, lame_lambda=lame_lambda, shear_mu=shear_mu, packed=packed, scales=scales, perm=perm)


courant = 0.15


def unpack(words):
    low = (words & 255) - 128
    middle = (jnp.right_shift(words, 8) & 255) - 128
    high = (jnp.right_shift(words, 16) & 255) - 128
    topmost = jnp.right_shift(words, 24)
    return jnp.concatenate([low, middle, high, topmost], axis=-1).astype(jnp.float32)


def inverse_order(row):
    count = row.shape[0]
    slots = jnp.arange(count, dtype=jnp.int32)
    hits = (row[None, :] == slots[:, None]).astype(jnp.int32)
    return jnp.sum(hits * slots[None, :], axis=1).astype(jnp.int32)


def forward_field(packed, scales, perm):
    comp = packed.shape[3]
    by_owner = jnp.swapaxes(packed, 0, 1)
    factors = jnp.swapaxes(scales, 0, 1)

    def one_owner(items):
        words, factor, row = items
        blocks = unpack(words) * factor[..., None]
        ordered = jnp.take(blocks, inverse_order(row), axis=0)
        return jnp.transpose(ordered, (2, 1, 0, 3)).reshape(comp, N_GY, CX, CY, CZ)

    whole_field = lax.map(one_owner, (by_owner, factors, perm))
    whole_field = jnp.transpose(whole_field, (1, 0, 3, 2, 4, 5))
    return whole_field.reshape(comp, NX, NY, NZ)


def step_ahead(field, axis):
    count = field.shape[axis]
    widths = [(0, 0)] * field.ndim
    widths[axis] = (0, 1)
    return jnp.pad(lax.slice_in_dim(field, 1, count, axis=axis), widths)


def step_behind(field, axis):
    count = field.shape[axis]
    widths = [(0, 0)] * field.ndim
    widths[axis] = (1, 0)
    return jnp.pad(lax.slice_in_dim(field, 0, count - 1, axis=axis), widths)


def diff_ahead(field, axis):
    return step_ahead(field, axis) - field


def diff_behind(field, axis):
    return field - step_behind(field, axis)


def move_velocity(velocity, stress, buoyancy):
    scaled = courant * buoyancy
    return [
        velocity[0] - scaled * (diff_ahead(stress[0], 0) + diff_behind(stress[3], 1) + diff_behind(stress[4], 2)),
        velocity[1] - scaled * (diff_behind(stress[3], 0) + diff_ahead(stress[1], 1) + diff_behind(stress[5], 2)),
        velocity[2] - scaled * (diff_behind(stress[4], 0) + diff_behind(stress[5], 1) + diff_ahead(stress[2], 2)),
    ]


def strains(velocity):
    return [
        diff_behind(velocity[0], 0),
        diff_behind(velocity[1], 1),
        diff_behind(velocity[2], 2),
        diff_ahead(velocity[0], 1) + diff_ahead(velocity[1], 0),
        diff_ahead(velocity[0], 2) + diff_ahead(velocity[2], 0),
        diff_ahead(velocity[1], 2) + diff_ahead(velocity[2], 1),
    ]


def move_stress(stress, strain, lame_lambda, shear_mu):
    trace = strain[0] + strain[1] + strain[2]
    result = []
    for index in range(3):
        result.append(stress[index] - courant * (lame_lambda * trace + 2.0 * shear_mu * strain[index]))
    for index in range(3, 6):
        result.append(stress[index] - courant * shear_mu * strain[index])
    return result


def reference(adjoint, buoyancy, lame_lambda, shear_mu, packed, scales, perm):
    forward = forward_field(packed, scales, perm)
    velocity = [adjoint[index] for index in range(3)]
    stress = [adjoint[index] for index in range(3, 9)]
    grad_lambda = jnp.zeros(buoyancy.shape, jnp.float32)
    grad_mu = jnp.zeros(buoyancy.shape, jnp.float32)
    for step in range(STEPS):
        velocity = move_velocity(velocity, stress, buoyancy)
        strain = strains(velocity)
        stress = move_stress(stress, strain, lame_lambda, shear_mu)
        stored = [forward[6 * step + index] for index in range(6)]
        trace = strain[0] + strain[1] + strain[2]
        grad_lambda = grad_lambda + trace * (stored[0] + stored[1] + stored[2])
        grad_mu = grad_mu + 2.0 * (strain[0] * stored[0] + strain[1] * stored[1] + strain[2] * stored[2])
        grad_mu = grad_mu + strain[3] * stored[3] + strain[4] * stored[4] + strain[5] * stored[5]
    return jnp.stack(velocity + stress), jnp.stack([grad_lambda, grad_mu])
```

```python
import functools

import jax
import jax.numpy as jnp
from jax import lax
from jax.experimental import pallas as pl
from jax.experimental.pallas import tpu as pltpu
from jax.sharding import PartitionSpec as P

MESH = pl.DeviceIdType.MESH
STEPS = 2
COURANT = 0.15
ROWS = 8
ZBIT = 8

VX, VY, VZ, SXX, SYY, SZZ, SXY, SXZ, SYZ = range(9)

DOWN_S, DOWN_V, DOWN_B, DOWN_C, UP_S, UP_V, UP_B, UP_C = range(8)
STRESS_Y = ((0, (SYY,), -1), (1, (SXY, SYZ), 1))
SPEED_Y = ((3, (VX, VZ), -1), (5, (VY,), 1))


def partner(me, distance, count):
    if count & (count - 1):
        return lax.rem(me + distance, count)
    result, bit = me, 1
    while bit < count:
        if distance & bit:
            result = result + bit - 2 * bit * ((me // bit) % 2)
        bit *= 2
    return result


def kernel(n_x, n_y, adj, buoy, lam, shear, packed, scales, perm, out, grads,
           cur, coef, strain, halo_x, halo_b, part, corner, corner_send, halo_y, send_y, late_y, late_send,
           table, scale_v, factor_send, factors, factor_s, perm_v, inv_v, inv,
           in_sem, xs_sem, xr_sem, ys_sem, yr_sem, ws_sem, wr_sem, fs_sem, fr_sem, loc_sem, *words):
    cx, cy, cz = buoy.shape
    comp = packed.shape[1]
    per_step = comp // STEPS
    lanes = packed.shape[3]
    segw = packed.shape[2] * lanes
    tiles = cy // ROWS
    last = cx - 1
    me_x, me_y = lax.axis_index("gx"), lax.axis_index("gy")

    barrier = pltpu.get_barrier_semaphore()
    for distance in range(1, n_x):
        pl.semaphore_signal(barrier, inc=1, device_id={"gx": partner(me_x, distance, n_x)}, device_id_type=MESH)

    def edge(way, axis):
        me, count = (me_x, n_x) if axis == "gx" else (me_y, n_y)
        return (me > 0) if way < 0 else (me < count - 1)

    for way in (-1, 1):
        @pl.when(edge(way, "gy"))
        def _():
            pl.semaphore_signal(barrier, inc=1, device_id={"gy": me_y + way}, device_id_type=MESH)

    loads = {}
    for index in (SXX, SXY, SXZ, SYY, SYZ, SZZ, VX, VY, VZ):
        loads[index] = pltpu.make_async_copy(adj.at[index], cur.at[index, pl.ds(1, cx)], in_sem.at[index])
    for index, ref in enumerate((buoy, lam, shear)):
        loads[9 + index] = pltpu.make_async_copy(ref, coef.at[index], in_sem.at[9 + index])
    load_perm = pltpu.make_async_copy(perm, perm_v, loc_sem.at[0])
    load_scales = pltpu.make_async_copy(scales, scale_v, loc_sem.at[1])
    own_words = [pltpu.make_async_copy(packed.at[me_x, pl.ds(step * per_step, per_step)], words[step].at[me_x],
                                       loc_sem.at[2 + step]) for step in range(STEPS)]
    for index in (9, SXY, SXZ, SYZ, SXX, SYY, SZZ, VX, VY, VZ, 10, 11):
        loads[index].start()
    load_perm.start()
    load_scales.start()
    for copy in own_words:
        copy.start()

    def x_copy(step, kind):
        way = 1 if kind < UP_S else -1
        if kind == DOWN_S:
            fields = pl.ds(SXY, 2)
            src = adj.at[fields, last] if step == 0 else cur.at[fields, cx]
            dst = halo_x.at[step, pl.ds(0, 2)]
        elif kind == DOWN_V:
            src, dst = part.at[step, pl.ds(0, 1)], halo_x.at[step, pl.ds(2, 1)]
        elif kind == DOWN_B:
            src, dst = buoy.at[last], halo_b.at[0]
        elif kind == DOWN_C:
            src, dst = corner_send.at[step, pl.ds(0, 1)], corner.at[step, pl.ds(0, 1)]
        elif kind == UP_S:
            src, dst = (adj.at[SXX, 0] if step == 0 else cur.at[SXX, 1]), halo_x.at[step, 3]
        elif kind == UP_V:
            src, dst = part.at[step, pl.ds(1, 2)], halo_x.at[step, pl.ds(4, 2)]
        elif kind == UP_B:
            src, dst = buoy.at[0], halo_b.at[1]
        else:
            src, dst = corner_send.at[step, pl.ds(1, 2)], corner.at[step, pl.ds(1, 2)]
        return way, pltpu.make_async_remote_copy(
            src_ref=src, dst_ref=dst, send_sem=xs_sem.at[step, kind], recv_sem=xr_sem.at[step, kind],
            device_id={"gx": me_x + way}, device_id_type=MESH)

    def x_start(step, *kinds):
        for kinds_way, way in ((kinds[:], 1), (kinds[:], -1)):
            mine = [k for k in kinds_way if (k < UP_S) == (way == 1)]
            if mine:
                @pl.when(edge(way, "gx"))
                def _():
                    for kind in mine:
                        x_copy(step, kind)[1].start()

    def x_wait(step, what, *kinds):
        for way in (1, -1):
            mine = [k for k in kinds if (k < UP_S) == (way == 1)]
            if mine:
                @pl.when(edge(-way if what == "recv" else way, "gx"))
                def _():
                    for kind in mine:
                        copy = x_copy(step, kind)[1]
                        if what == "recv":
                            copy.wait_recv()
                        else:
                            copy.wait_send()

    def y_copy(step, message):
        start, fields, way = message
        slot = 6 * step + start
        return pltpu.make_async_remote_copy(
            src_ref=send_y.at[pl.ds(slot, len(fields))], dst_ref=halo_y.at[pl.ds(slot, len(fields))],
            send_sem=ys_sem.at[slot], recv_sem=yr_sem.at[slot],
            device_id={"gy": me_y + way}, device_id_type=MESH)

    def late(step, which):
        way = -1 if which == 0 else 1
        first, count = (3 * step, 2) if which == 0 else (3 * step + 2, 1)
        sem = 6 * STEPS + 2 * step + which
        return way, pltpu.make_async_remote_copy(
            src_ref=late_send.at[pl.ds(first, count)], dst_ref=late_y.at[pl.ds(first, count)],
            send_sem=ys_sem.at[sem], recv_sem=yr_sem.at[sem],
            device_id={"gy": me_y + way}, device_id_type=MESH)

    def send_rows(step, messages):
        for message in messages:
            start, fields, way = message

            @pl.when(edge(way, "gy"))
            def _():
                row = 0 if way < 0 else cy - 1
                for offset, field in enumerate(fields):
                    for x in range(cx):
                        send_y[6 * step + start + offset, pl.ds(x, 1), :] = cur[field, 1 + x, pl.ds(row, 1), :]
                y_copy(step, message).start()

    def receive_y(step, messages):
        for message in messages:
            @pl.when(edge(-message[2], "gy"))
            def _():
                y_copy(step, message).wait_recv()

    def send_late(step):
        @pl.when(edge(-1, "gy"))
        def _():
            late_send[3 * step] = cur[VX, cx, pl.ds(0, 1), :]
            late_send[3 * step + 1] = cur[VZ, 1, pl.ds(0, 1), :]
            late(step, 0)[1].start()

        @pl.when(edge(1, "gy"))
        def _():
            late_send[3 * step + 2] = cur[VY, 1, pl.ds(cy - 1, 1), :]
            late(step, 1)[1].start()

    def receive_late(step):
        @pl.when(edge(1, "gy"))
        def _():
            late(step, 0)[1].wait_recv()
            halo_y[6 * step + 3, pl.ds(last, 1), :] = late_y[3 * step]
            halo_y[6 * step + 4, pl.ds(0, 1), :] = late_y[3 * step + 1]

        @pl.when(edge(-1, "gy"))
        def _():
            late(step, 1)[1].wait_recv()
            halo_y[6 * step + 5, pl.ds(0, 1), :] = late_y[3 * step + 2]

    def forward_corners(step):
        slot = 6 * step
        corner_send[step, 0] = halo_y[slot + 1, pl.ds(last, 1), :]
        corner_send[step, 1] = halo_y[slot, pl.ds(0, 1), :]
        corner_send[step, 2] = halo_y[slot + 2, pl.ds(0, 1), :]
        x_start(step, DOWN_C, UP_C)

    def word_copy(distance, step):
        to = partner(me_x, distance, n_x)
        stored = pl.ds(step * per_step, per_step)
        return pltpu.make_async_remote_copy(
            src_ref=packed.at[to, stored], dst_ref=words[step].at[me_x], send_sem=ws_sem.at[distance, step],
            recv_sem=wr_sem.at[distance, step], device_id={"gx": to}, device_id_type=MESH)

    def factor_copy(distance):
        to = partner(me_x, distance, n_x)
        return pltpu.make_async_remote_copy(
            src_ref=factor_send.at[to], dst_ref=factors.at[me_x], send_sem=fs_sem.at[distance],
            recv_sem=fr_sem.at[distance], device_id={"gx": to}, device_id_type=MESH)

    far = [d for d in range(1, n_x) if d & ZBIT]
    near = [d for d in range(1, n_x) if not d & ZBIT]

    def send_words(step, distances):
        for distance in distances:
            word_copy(distance, step).start()

    def receive_words(step):
        own_words[step].wait()
        for distance in near + far:
            word_copy(distance, step).wait()

    sub = lax.broadcasted_iota(jnp.int32, (ROWS, cz), 0)
    lane = lax.broadcasted_iota(jnp.int32, (ROWS, cz), 1)
    first_row, last_row = sub == 0, sub == ROWS - 1
    first_lane, last_lane = lane == 0, lane == cz - 1

    def tile(field, x, t):
        return cur[field, x + 1, pl.ds(t * ROWS, ROWS), :]

    def z_before(value):
        return jnp.where(first_lane, 0.0, pltpu.roll(value, 1, 1))

    def z_after(value):
        return jnp.where(last_lane, 0.0, pltpu.roll(value, cz - 1, 1))

    def y_before(value, field, x, t, slot):
        if t == 0:
            row = None if slot is None else halo_y[slot, pl.ds(x, 1), :]
        else:
            row = cur[field, x + 1, pl.ds(t * ROWS - 1, 1), :]
        row = 0.0 if row is None else jnp.broadcast_to(row, value.shape)
        return jnp.where(first_row, row, pltpu.roll(value, 1, 0))

    def y_after(value, field, x, t, slot):
        if t == tiles - 1:
            row = None if slot is None else halo_y[slot, pl.ds(x, 1), :]
        else:
            row = cur[field, x + 1, pl.ds(t * ROWS + ROWS, 1), :]
        row = 0.0 if row is None else jnp.broadcast_to(row, value.shape)
        return jnp.where(last_row, row, pltpu.roll(value, ROWS - 1, 0))

    def keep(step, field, x, rows, value):
        cur[field, x + 1, rows, :] = value
        if step == STEPS - 1:
            out[field, x, rows, :] = value

    def partials(step):
        for t in range(tiles):
            rows = pl.ds(t * ROWS, ROWS)
            sxx, sxy, sxz = tile(SXX, last, t), tile(SXY, last, t), tile(SXZ, last, t)
            part[step, 0, rows, :] = tile(VX, last, t) - (COURANT * coef[0, last, rows, :]) * (
                (sxy - y_before(sxy, SXY, last, t, None)) + (sxz - z_before(sxz)) - sxx)
        for t in range(tiles):
            rows = pl.ds(t * ROWS, ROWS)
            scaled = COURANT * coef[0, 0, rows, :]
            sxy, sxz, syz = tile(SXY, 0, t), tile(SXZ, 0, t), tile(SYZ, 0, t)
            syy, szz = tile(SYY, 0, t), tile(SZZ, 0, t)
            part[step, 1, rows, :] = tile(VY, 0, t) - scaled * (
                sxy + (y_after(syy, SYY, 0, t, None) - syy) + (syz - z_before(syz)))
            part[step, 2, rows, :] = tile(VZ, 0, t) - scaled * (
                sxz + (syz - y_before(syz, SYZ, 0, t, None)) + (z_after(szz) - szz))

    def velocity(step, which, x, want=(VX, VY, VZ)):
        slot = 6 * step
        for t in which:
            rows = pl.ds(t * ROWS, ROWS)
            scaled = COURANT * coef[0, x, rows, :]
            sxy, sxz = tile(SXY, x, t), tile(SXZ, x, t)
            if VX in want:
                keep(step, VX, x, rows, tile(VX, x, t) - scaled * (
                    (tile(SXX, x + 1, t) - tile(SXX, x, t)) + (sxy - y_before(sxy, SXY, x, t, slot + 1))
                    + (sxz - z_before(sxz))))
            if VY in want:
                syy, syz, szz = tile(SYY, x, t), tile(SYZ, x, t), tile(SZZ, x, t)
                keep(step, VY, x, rows, tile(VY, x, t) - scaled * (
                    (sxy - tile(SXY, x - 1, t)) + (y_after(syy, SYY, x, t, slot) - syy) + (syz - z_before(syz))))
                keep(step, VZ, x, rows, tile(VZ, x, t) - scaled * (
                    (sxz - tile(SXZ, x - 1, t)) + (syz - y_before(syz, SYZ, x, t, slot + 2)) + (z_after(szz) - szz)))

    def complete(step):
        slot = 6 * step
        for t in range(tiles):
            rows = pl.ds(t * ROWS, ROWS)

            def edge_row(value, row, at):
                return value + jnp.where(at, jnp.broadcast_to(row, (ROWS, cz)), 0.0)

            scaled = COURANT * coef[0, last, rows, :]
            more = halo_x[step, 3, rows, :]
            if t == 0:
                more = edge_row(more, -halo_y[slot + 1, pl.ds(last, 1), :], first_row)
            keep(step, VX, last, rows, part[step, 0, rows, :] - scaled * more)

            scaled = COURANT * coef[0, 0, rows, :]
            more = halo_x[step, 0, rows, :]
            if t == tiles - 1:
                more = edge_row(more, -halo_y[slot, pl.ds(0, 1), :], last_row)
            keep(step, VY, 0, rows, part[step, 1, rows, :] + scaled * more)
            more = halo_x[step, 1, rows, :]
            if t == 0:
                more = edge_row(more, halo_y[slot + 2, pl.ds(0, 1), :], first_row)
            keep(step, VZ, 0, rows, part[step, 2, rows, :] + scaled * more)

            more = tile(SXX, 0, t)
            if t == 0:
                more = edge_row(more, -corner[step, 0], first_row)
            cur[VX, 0, rows, :] = halo_x[step, 2, rows, :] - (COURANT * halo_b[0, rows, :]) * more

            scaled = COURANT * halo_b[1, rows, :]
            more = tile(SXY, last, t)
            if t == tiles - 1:
                more = edge_row(more, -corner[step, 1], last_row)
            cur[VY, cx + 1, rows, :] = halo_x[step, 4, rows, :] + scaled * more
            more = tile(SXZ, last, t)
            if t == 0:
                more = edge_row(more, corner[step, 2], first_row)
            cur[VZ, cx + 1, rows, :] = halo_x[step, 5, rows, :] + scaled * more

    def stress(step, which, x):
        slot = 6 * step + 3
        for t in which:
            rows = pl.ds(t * ROWS, ROWS)
            vx, vy, vz = tile(VX, x, t), tile(VY, x, t), tile(VZ, x, t)
            exx = vx - tile(VX, x - 1, t)
            eyy = vy - y_before(vy, VY, x, t, slot + 2)
            ezz = vz - z_before(vz)
            exy = (y_after(vx, VX, x, t, slot) - vx) + (tile(VY, x + 1, t) - vy)
            exz = (z_after(vx) - vx) + (tile(VZ, x + 1, t) - vz)
            eyz = (z_after(vy) - vy) + (y_after(vz, VZ, x, t, slot + 1) - vz)
            both = (exx, eyy, ezz, exy, exz, eyz)
            for index, value in enumerate(both):
                strain[6 * step + index, x, rows, :] = value
            pull = (COURANT * coef[1, x, rows, :]) * (exx + eyy + ezz)
            mu = COURANT * coef[2, x, rows, :]
            for index, value in enumerate(both):
                change = pull + (2.0 * mu) * value if index < 3 else mu * value
                moved = tile(SXX + index, x, t) - change
                if step == STEPS - 1:
                    out[SXX + index, x, rows, :] = moved
                else:
                    cur[SXX + index, x + 1, rows, :] = moved

    def over(first, stop, body):
        def run(x, carry):
            body(x)
            return carry
        lax.fori_loop(first, stop, run, 0)

    def ends(body):
        def run(index, carry):
            body(index * (cx - 1))
            return carry
        lax.fori_loop(0, 2, run, 0)

    width = lanes
    per_x = cy * cz // (4 * segw)

    def source(row, chunk):
        offset = row * cz + chunk * width
        within = offset % (4 * segw)
        return offset // (4 * segw), within % segw, within // segw

    sub_w = lax.broadcasted_iota(jnp.int32, (ROWS, width), 0)

    def gradient(step, x):
        made = {}
        for t in range(tiles):
            for chunk in range(cz // width):
                rows = pl.ds(t * ROWS, ROWS)
                columns = pl.ds(chunk * width, width)
                plan = [source(t * ROWS + r, chunk) for r in range(ROWS)]
                shift = jnp.full((ROWS, width), 8 * plan[0][2], jnp.int32)
                for r in range(1, ROWS):
                    if plan[r][2] != plan[r - 1][2]:
                        shift = jnp.where(sub_w >= r, 8 * plan[r][2], shift)
                key = tuple(p[:2] for p in plan)
                distinct = list(dict.fromkeys(key))
                masks = []
                for item in distinct[1:]:
                    mask = None
                    for r in range(ROWS):
                        if key[r] == item:
                            mask = (sub_w == r) if mask is None else mask | (sub_w == r)
                    masks.append(mask)
                holders = {b: inv[0, x * per_x + b] for b in dict.fromkeys(k[0] for k in key)}
                blocks = [k[0] for k in key]

                def stored(c):
                    if (key, c) not in made:
                        word = None
                        for position, (block, start) in enumerate(distinct):
                            piece = jnp.broadcast_to(
                                words[step][holders[block], c - per_step * step, pl.ds(start // lanes, 1), :], (ROWS, width))
                            word = piece if word is None else jnp.where(masks[position - 1], piece, word)
                        made[key, c] = word ^ jnp.int32(-2147483648)
                    byte = (lax.shift_right_logical(made[key, c], shift) & 255) - 128
                    factor = None
                    for r in range(ROWS):
                        if r == 0:
                            factor = factor_s[holders[blocks[0]], 0, c]
                        elif blocks[r] != blocks[r - 1]:
                            factor = jnp.where(sub_w >= r, factor_s[holders[blocks[r]], 0, c], factor)
                    return byte.astype(jnp.float32) * factor

                e = [strain[6 * step + index, x, rows, columns] for index in range(6)]
                f = [stored(6 * step + index) for index in range(6)]
                grad_lambda = (e[0] + e[1] + e[2]) * (f[0] + f[1] + f[2])
                grad_mu = 2.0 * (e[0] * f[0] + e[1] * f[1] + e[2] * f[2])
                grad_mu = grad_mu + e[3] * f[3] + e[4] * f[4] + e[5] * f[5]
                if step > 0:
                    grad_lambda = grads[0, x, rows, columns] + grad_lambda
                    grad_mu = grads[1, x, rows, columns] + grad_mu
                grads[0, x, rows, columns] = grad_lambda
                grads[1, x, rows, columns] = grad_mu

    for way in (-1, 1):
        @pl.when(jnp.logical_not(edge(way, "gx")))
        def _():
            zero = jnp.zeros((ROWS, cz), jnp.float32)
            for t in range(tiles):
                rows = pl.ds(t * ROWS, ROWS)
                halo_b[0 if way < 0 else 1, rows, :] = zero
                for step in range(STEPS):
                    for slot in (0, 1, 2) if way < 0 else (3, 4, 5):
                        halo_x[step, slot, rows, :] = zero
            for step in range(STEPS):
                for slot in (0,) if way < 0 else (1, 2):
                    corner[step, slot] = jnp.zeros((1, cz), jnp.float32)

        @pl.when(jnp.logical_not(edge(way, "gy")))
        def _():
            for step in range(STEPS):
                for start, fields, sent in STRESS_Y + SPEED_Y:
                    if sent == -way:
                        for offset in range(len(fields)):
                            halo_y[6 * step + start + offset] = jnp.zeros((cx, cz), jnp.float32)

    outer = (0, tiles - 1) if tiles > 1 else (0,)
    inner = range(1, tiles - 1)
    every = range(tiles)
    waited = set()

    def need(*which):
        for index in which:
            if index not in waited:
                loads[index].wait()
                waited.add(index)

    need(*range(12))
    partials(0)

    pl.semaphore_wait(barrier, n_x - 1 + jnp.minimum(me_y, 1) + jnp.minimum(n_y - 1 - me_y, 1))

    x_start(0, DOWN_S, UP_S, DOWN_V, UP_V, DOWN_B, UP_B)
    send_rows(0, STRESS_Y)
    send_words(0, near)

    load_scales.wait()
    load_perm.wait()
    square = 128
    sub_q = lax.broadcasted_iota(jnp.int32, (square, square), 0)
    lane_q = lax.broadcasted_iota(jnp.int32, (square, square), 1)
    table[...] = jnp.zeros((16, square), jnp.float32)
    for c in range(comp):
        table[pl.ds(c, 1), pl.ds(0, n_x)] = scale_v[c]
    by_owner = jnp.transpose(jnp.concatenate([table[...], jnp.zeros((square - 16, square), jnp.float32)], axis=0))
    for owner in range(n_x):
        factor_send[owner] = by_owner[owner:owner + 1, :comp]
    inv_v[...] = jnp.full((1, square), -1, jnp.int32)
    inv_v[pl.ds(0, 1), pl.ds(0, n_x)] = perm_v[...]
    by_holder = jnp.transpose(jnp.broadcast_to(inv_v[...], (square, square)))
    inv_v[...] = jnp.max(jnp.where(by_holder == lane_q, sub_q, 0), axis=0, keepdims=True)
    inverse = pltpu.make_async_copy(inv_v, inv, loc_sem.at[0])
    inverse.start()
    own_factor = pltpu.make_async_copy(factor_send.at[me_x], factors.at[me_x], loc_sem.at[1])
    own_factor.start()

    half = len(far) // 2
    for step in range(STEPS):
        if step > 0:
            partials(step)
            x_start(step, DOWN_S, UP_S, DOWN_V, UP_V)
            send_rows(step, STRESS_Y)
            send_words(step, far)
            send_words(step, near)
        receive_y(step, STRESS_Y)
        forward_corners(step)
        velocity(step, every, 0, (VX,))
        velocity(step, every, last, (VY, VZ))
        over(1, last, functools.partial(velocity, step, every))
        send_rows(step, SPEED_Y)
        if step == 0:
            send_words(0, far[:half])
            for distance in near + far:
                factor_copy(distance).start()
        receive_y(step, SPEED_Y)
        over(1, last, functools.partial(stress, step, every))
        if step > 0:
            own_factor.wait()
            for distance in near + far:
                factor_copy(distance).wait()
            to_scalar = pltpu.make_async_copy(factors, factor_s, loc_sem.at[1])
            to_scalar.start()
            to_scalar.wait()
            inverse.wait()
            receive_words(step - 1)
            over(0, cx, functools.partial(gradient, step - 1))
        x_wait(step, "recv", DOWN_S, DOWN_V, DOWN_C, UP_S, UP_V, UP_C)
        if step == 0:
            x_wait(0, "recv", DOWN_B, UP_B)
        complete(step)
        send_late(step)
        if step == 0:
            send_words(0, far[half:])
        ends(functools.partial(stress, step, inner))
        receive_late(step)
        ends(functools.partial(stress, step, outer))
    receive_words(STEPS - 1)
    over(0, cx, functools.partial(gradient, STEPS - 1))

    for step in range(STEPS):
        x_wait(step, "send", DOWN_S, DOWN_V, DOWN_C, UP_S, UP_V, UP_C)
        for message in STRESS_Y + SPEED_Y:
            @pl.when(edge(message[2], "gy"))
            def _():
                y_copy(step, message).wait_send()
        for which in (0, 1):
            way, copy = late(step, which)

            @pl.when(edge(way, "gy"))
            def _():
                copy.wait_send()
    x_wait(0, "send", DOWN_B, UP_B)


def on_device(n_x, n_y, adjoint, buoyancy, lame_lambda, shear_mu, packed, scales, perm):
    fields, cx, cy, cz = adjoint.shape
    comp, segw = packed.shape[3:]
    lanes = min(128, segw)
    packed = packed.reshape(n_x, comp, segw // lanes, lanes)
    scales = jnp.transpose(scales, (0, 3, 2, 1)).reshape(comp, 1, n_x)
    halos = 6 * STEPS
    dma = pltpu.SemaphoreType.DMA
    f32, i32 = jnp.float32, jnp.int32
    return pl.pallas_call(
        functools.partial(kernel, n_x, n_y),
        out_shape=(pltpu.VMEM(adjoint.shape, f32), pltpu.VMEM((2, cx, cy, cz), f32)),
        in_specs=[pl.BlockSpec(memory_space=pltpu.HBM)] * 7,
        out_specs=(pl.BlockSpec(memory_space=pltpu.VMEM),) * 2,
        scratch_shapes=[
            pltpu.VMEM((fields, cx + 2, cy, cz), f32),
            pltpu.VMEM((3, cx, cy, cz), f32),
            pltpu.VMEM((comp, cx, cy, cz), f32),
            pltpu.VMEM((STEPS, 6, cy, cz), f32),
            pltpu.VMEM((2, cy, cz), f32),
            pltpu.VMEM((STEPS, 3, cy, cz), f32),
            pltpu.VMEM((STEPS, 3, 1, cz), f32),
            pltpu.VMEM((STEPS, 3, 1, cz), f32),
            pltpu.VMEM((halos, cx, cz), f32),
            pltpu.VMEM((halos, cx, cz), f32),
            pltpu.VMEM((3 * STEPS, 1, cz), f32),
            pltpu.VMEM((3 * STEPS, 1, cz), f32),
            pltpu.VMEM((16, 128), f32),
            pltpu.VMEM((comp, 1, n_x), f32),
            pltpu.VMEM((n_x, 1, comp), f32),
            pltpu.VMEM((n_x, 1, comp), f32),
            pltpu.SMEM((n_x, 1, comp), f32),
            pltpu.VMEM((1, n_x), i32),
            pltpu.VMEM((1, 128), i32),
            pltpu.SMEM((1, 128), i32),
            dma((12,)), dma((STEPS, 8)), dma((STEPS, 8)), dma((halos + 2 * STEPS,)), dma((halos + 2 * STEPS,)),
            dma((n_x, STEPS)), dma((n_x, STEPS)), dma((n_x,)), dma((n_x,)), dma((2 + STEPS,)),
        ] + [pltpu.VMEM((n_x, comp // STEPS, segw // lanes, lanes), i32)] * STEPS,
        compiler_params=pltpu.CompilerParams(collective_id=0, has_side_effects=True,
                                             vmem_limit_bytes=64000000),
    )(adjoint, buoyancy, lame_lambda, shear_mu, packed, scales, perm)


def solution(mesh):
    return jax.shard_map(
        functools.partial(on_device, mesh.shape["gx"], mesh.shape["gy"]),
        mesh=mesh,
        in_specs=(
            P(None, "gx", "gy", None),
            P("gx", "gy", None),
            P("gx", "gy", None),
            P("gx", "gy", None),
            P("gx", None, "gy", None, None),
            P("gx", None, "gy", None),
            P("gx", None),
        ),
        out_specs=(P(None, "gx", "gy", None), P(None, "gx", "gy", None)),
        check_vma=False,
    )
```

```python
import functools

import jax
import jax.numpy as jnp
from jax import lax
from jax.experimental import pallas as pl
from jax.experimental.pallas import tpu as pltpu
from jax.sharding import PartitionSpec as P

MESH = pl.DeviceIdType.MESH
STEPS = 2
COURANT = 0.15
ROWS = 8
ZBIT = 8
PAIR = 2

VX, VY, VZ, SXX, SYY, SZZ, SXY, SXZ, SYZ = range(9)

DOWN_S, DOWN_V, DOWN_B, UP_S, UP_V, UP_B = range(6)
Y_SLOTS = 6
Y_SYY, Y_SXY, Y_SYZ, Y_VX, Y_VZ, Y_VY = range(Y_SLOTS)
STRESS_Y = ((Y_SYY, 1, -1), (Y_SXY, 2, 1))
SPEED_Y = ((Y_VX, 2, -1), (Y_VY, 1, 1))
BUOY_Y = ((0, 1, -1), (1, 1, 1))
C_SXY, C_SXZ, C_SYY, C_SXX, C_SYZ = range(5)
CORNERS = ((1, 1, C_SXY, ((SXY, 1, 1),)), (1, -1, C_SXZ, ((SXZ, 1, 0),)),
           (-1, -1, C_SYY, ((SYY, 0, 0), (SXX, 0, 0))), (-1, 1, C_SYZ, ((SYZ, 0, 1),)))


def partner(me, distance, count):
    if count & (count - 1):
        return lax.rem(me + distance, count)
    result, bit = me, 1
    while bit < count:
        if distance & bit:
            result = result + bit - 2 * bit * ((me // bit) % 2)
        bit *= 2
    return result


def kernel(n_x, n_y, adj, buoy, lam, shear, packed, scales, perm, out, grads,
           cur, coef, strain, halo_x, halo_b, part, corner, corner_send, halo_y, send_y,
           relay, table, scale_v, factor_send, factors, factor_s, perm_v, inv_v, inv,
           in_sem, xs_sem, xr_sem, cs_sem, cr_sem, rs_sem, rr_sem, ys_sem, yr_sem, ws_sem, wr_sem, fs_sem, fr_sem, loc_sem, *words):
    cx, cy, cz = buoy.shape
    comp = packed.shape[1]
    per_step = comp // STEPS
    lanes = packed.shape[3]
    segw = packed.shape[2] * lanes
    tiles = cy // ROWS
    last = cx - 1
    me_x, me_y = lax.axis_index("gx"), lax.axis_index("gy")

    barrier = pltpu.get_barrier_semaphore()
    for distance in range(1, n_x):
        pl.semaphore_signal(barrier, inc=1, device_id={"gx": partner(me_x, distance, n_x)}, device_id_type=MESH)

    def edge(way, axis):
        me, count = (me_x, n_x) if axis == "gx" else (me_y, n_y)
        return (me > 0) if way < 0 else (me < count - 1)

    for way in (-1, 1):
        @pl.when(edge(way, "gy"))
        def _():
            pl.semaphore_signal(barrier, inc=1, device_id={"gy": me_y + way}, device_id_type=MESH)

        for way_x in (-1, 1):
            @pl.when(edge(way, "gy") & edge(way_x, "gx"))
            def _():
                pl.semaphore_signal(barrier, inc=1, device_id={"gx": me_x + way_x, "gy": me_y + way},
                                    device_id_type=MESH)

    loads = {}
    for index in (SXX, SXY, SXZ, SYY, SYZ, SZZ, VX, VY, VZ):
        loads[index] = pltpu.make_async_copy(adj.at[index], cur.at[index, pl.ds(1, cx)], in_sem.at[index])
    for index, ref in enumerate((buoy, lam, shear)):
        loads[9 + index] = pltpu.make_async_copy(ref, coef.at[index], in_sem.at[9 + index])
    load_perm = pltpu.make_async_copy(perm, perm_v, loc_sem.at[0])
    load_scales = pltpu.make_async_copy(scales, scale_v, loc_sem.at[1])
    own_words = [pltpu.make_async_copy(packed.at[me_x, pl.ds(step * per_step, per_step)], words[step].at[me_x],
                                       loc_sem.at[2 + step]) for step in range(STEPS)]
    for index in (9, SXY, SXZ, SYZ, SXX, SYY, SZZ, VX, VY, VZ, 10, 11):
        loads[index].start()
    load_perm.start()
    load_scales.start()
    for copy in own_words:
        copy.start()

    def x_copy(step, kind):
        way = 1 if kind < UP_S else -1
        if kind == DOWN_S:
            fields = pl.ds(SXY, 2)
            src = adj.at[fields, last] if step == 0 else cur.at[fields, cx]
            dst = halo_x.at[step, pl.ds(0, 2)]
        elif kind == DOWN_V:
            src, dst = part.at[step, pl.ds(0, 1)], halo_x.at[step, pl.ds(2, 1)]
        elif kind == DOWN_B:
            src, dst = buoy.at[last], halo_b.at[0]
        elif kind == UP_S:
            src, dst = (adj.at[SXX, 0] if step == 0 else cur.at[SXX, 1]), halo_x.at[step, 3]
        elif kind == UP_V:
            src, dst = part.at[step, pl.ds(1, 2)], halo_x.at[step, pl.ds(4, 2)]
        else:
            src, dst = buoy.at[0], halo_b.at[1]
        return way, pltpu.make_async_remote_copy(
            src_ref=src, dst_ref=dst, send_sem=xs_sem.at[step, kind], recv_sem=xr_sem.at[step, kind],
            device_id={"gx": me_x + way}, device_id_type=MESH)

    def x_start(step, *kinds):
        for kinds_way, way in ((kinds[:], 1), (kinds[:], -1)):
            mine = [k for k in kinds_way if (k < UP_S) == (way == 1)]
            if mine:
                @pl.when(edge(way, "gx"))
                def _():
                    for kind in mine:
                        x_copy(step, kind)[1].start()

    def x_wait(step, what, *kinds):
        for way in (1, -1):
            mine = [k for k in kinds if (k < UP_S) == (way == 1)]
            if mine:
                @pl.when(edge(-way if what == "recv" else way, "gx"))
                def _():
                    for kind in mine:
                        copy = x_copy(step, kind)[1]
                        if what == "recv":
                            copy.wait_recv()
                        else:
                            copy.wait_send()

    def y_copy(step, message):
        start, count, way = message
        slot = Y_SLOTS * step + start
        return pltpu.make_async_remote_copy(
            src_ref=send_y.at[pl.ds(slot, count)], dst_ref=halo_y.at[pl.ds(slot, count)],
            send_sem=ys_sem.at[slot], recv_sem=yr_sem.at[slot],
            device_id={"gy": me_y + way}, device_id_type=MESH)

    def y_start(step, message):
        y_copy(step, message).start()

    def receive_y(step, messages):
        for message in messages:
            @pl.when(edge(-message[2], "gy"))
            def _():
                y_copy(step, message).wait_recv()

    def row_of(field, x, row):
        return cur[field, 1 + x, pl.ds(row, 1), :]

    def send_buoy_y():
        @pl.when(edge(-1, "gy"))
        def _():
            send_y[Y_SLOTS * STEPS, pl.ds(0, 1), :] = coef[0, last, pl.ds(0, 1), :]
            send_y[Y_SLOTS * STEPS, pl.ds(1, 1), :] = coef[0, 0, pl.ds(0, 1), :]
            y_start(STEPS, BUOY_Y[0])

        @pl.when(edge(1, "gy"))
        def _():
            send_y[Y_SLOTS * STEPS + 1, pl.ds(0, 1), :] = coef[0, 0, pl.ds(cy - 1, 1), :]
            y_start(STEPS, BUOY_Y[1])

    def send_stress_y(step):
        slot = Y_SLOTS * step

        @pl.when(edge(-1, "gy"))
        def _():
            for x in range(cx):
                send_y[slot + Y_SYY, pl.ds(x, 1), :] = row_of(SYY, x, 0)
            y_start(step, STRESS_Y[0])

        @pl.when(edge(1, "gy"))
        def _():
            for x in range(cx):
                send_y[slot + Y_SXY, pl.ds(x, 1), :] = row_of(SXY, x, cy - 1)
                send_y[slot + Y_SYZ, pl.ds(x, 1), :] = row_of(SYZ, x, cy - 1)
            y_start(step, STRESS_Y[1])

    def send_speed_y(step):
        slot = Y_SLOTS * step

        @pl.when(edge(-1, "gy"))
        def _():
            first = pl.ds(0, 1)
            for x in range(last):
                send_y[slot + Y_VX, pl.ds(x, 1), :] = row_of(VX, x, 0)
                send_y[slot + Y_VZ, pl.ds(x + 1, 1), :] = row_of(VZ, x + 1, 0)
            send_y[slot + Y_VX, pl.ds(last, 1), :] = part[step, 0, first, :] + (
                COURANT * coef[0, last, first, :]) * halo_y[slot + Y_SXY, pl.ds(last, 1), :]
            send_y[slot + Y_VZ, pl.ds(0, 1), :] = part[step, 2, first, :] + (
                COURANT * coef[0, 0, first, :]) * halo_y[slot + Y_SYZ, pl.ds(0, 1), :]
            y_start(step, SPEED_Y[0])

        @pl.when(edge(1, "gy"))
        def _():
            end = pl.ds(cy - 1, 1)
            for x in range(1, cx):
                send_y[slot + Y_VY, pl.ds(x, 1), :] = row_of(VY, x, cy - 1)
            send_y[slot + Y_VY, pl.ds(0, 1), :] = part[step, 1, end, :] - (
                COURANT * coef[0, 0, end, :]) * halo_y[slot + Y_SYY, pl.ds(0, 1), :]
            y_start(step, SPEED_Y[1])

    def fix_rows(step):
        slot, extra = Y_SLOTS * step, Y_SLOTS * STEPS
        one, end = pl.ds(0, 1), pl.ds(last, 1)
        halo_y[slot + Y_VX, end, :] = halo_y[slot + Y_VX, end, :] - (
            COURANT * halo_y[extra, one, :]) * corner[step, C_SXX]
        halo_y[slot + Y_VZ, one, :] = halo_y[slot + Y_VZ, one, :] + (
            COURANT * halo_y[extra, pl.ds(1, 1), :]) * corner[step, C_SXZ]
        halo_y[slot + Y_VY, one, :] = halo_y[slot + Y_VY, one, :] + (
            COURANT * halo_y[extra + 1, one, :]) * corner[step, C_SXY]

    def both_edges(way_x, way_y):
        return edge(way_x, "gx") & edge(way_y, "gy")

    def corner_copy(step, which):
        way_x, way_y, first, fields = CORNERS[which]
        slots = pl.ds(first, len(fields))
        return pltpu.make_async_remote_copy(
            src_ref=corner_send.at[step, slots], dst_ref=corner.at[step, slots],
            send_sem=cs_sem.at[step, which], recv_sem=cr_sem.at[step, which],
            device_id={"gx": me_x + way_x, "gy": me_y + way_y}, device_id_type=MESH)

    def send_corners(step):
        for which, (way_x, way_y, first, fields) in enumerate(CORNERS):
            @pl.when(both_edges(way_x, way_y))
            def _():
                for offset, (field, layer, row) in enumerate(fields):
                    corner_send[step, first + offset] = row_of(field, layer * last, row * (cy - 1))
                corner_copy(step, which).start()

    def receive_corners(step):
        for which, (way_x, way_y, first, fields) in enumerate(CORNERS):
            @pl.when(both_edges(-way_x, -way_y))
            def _():
                corner_copy(step, which).wait_recv()

    def word_copy(distance, step):
        to = partner(me_x, distance, n_x)
        stored = pl.ds(step * per_step, per_step)
        return pltpu.make_async_remote_copy(
            src_ref=packed.at[to, stored], dst_ref=words[step].at[me_x], send_sem=ws_sem.at[distance, step],
            recv_sem=wr_sem.at[distance, step], device_id={"gx": to}, device_id_type=MESH)

    def factor_copy(distance):
        to = partner(me_x, distance, n_x)
        return pltpu.make_async_remote_copy(
            src_ref=factor_send.at[to], dst_ref=factors.at[me_x], send_sem=fs_sem.at[distance],
            recv_sem=fr_sem.at[distance], device_id={"gx": to}, device_id_type=MESH)

    far = [d for d in range(1, n_x) if d & ZBIT]
    near = [d for d in range(1, n_x) if not d & ZBIT]

    outside = ((me_x // 2) % 4 == 0) | ((me_x // 2) % 4 == 3)
    inside = jnp.logical_not(outside)
    relayed = [(0, d) for d in far[:16]]

    def relay_in(index):
        step, distance = relayed[index]
        to = partner(me_x, distance, n_x)
        return pltpu.make_async_remote_copy(
            src_ref=packed.at[to, pl.ds(step * per_step, per_step)], dst_ref=relay.at[index],
            send_sem=ws_sem.at[distance, step], recv_sem=rr_sem.at[index],
            device_id={"gx": partner(me_x, PAIR, n_x)}, device_id_type=MESH)

    def relay_out(index):
        step, distance = relayed[index]
        return pltpu.make_async_remote_copy(
            src_ref=relay.at[index], dst_ref=words[step].at[partner(me_x, PAIR, n_x)],
            send_sem=rs_sem.at[index], recv_sem=wr_sem.at[distance, step],
            device_id={"gx": partner(me_x, distance ^ PAIR, n_x)}, device_id_type=MESH)

    def send_relays():
        @pl.when(outside)
        def _():
            for index in range(len(relayed)):
                relay_in(index).start()

    def pass_relays():
        @pl.when(inside)
        def _():
            for index in range(len(relayed)):
                relay_in(index).wait_recv()
                relay_out(index).start()

    def finish_relays():
        @pl.when(inside)
        def _():
            for index in range(len(relayed)):
                relay_out(index).wait_send()

    def words_of(out_words, in_words):
        @pl.when(outside)
        def _():
            for step, distances in out_words:
                send_words(step, [d for d in distances if (step, d) not in relayed])

        @pl.when(inside)
        def _():
            for step, distances in in_words:
                send_words(step, distances)

    def send_words(step, distances):
        for distance in distances:
            word_copy(distance, step).start()

    def receive_words(step):
        own_words[step].wait()
        for distance in near + far:
            word_copy(distance, step).wait()

    sub = lax.broadcasted_iota(jnp.int32, (ROWS, cz), 0)
    lane = lax.broadcasted_iota(jnp.int32, (ROWS, cz), 1)
    first_row, last_row = sub == 0, sub == ROWS - 1
    first_lane, last_lane = lane == 0, lane == cz - 1

    def tile(field, x, t):
        return cur[field, x + 1, pl.ds(t * ROWS, ROWS), :]

    def z_before(value):
        return jnp.where(first_lane, 0.0, pltpu.roll(value, 1, 1))

    def z_after(value):
        return jnp.where(last_lane, 0.0, pltpu.roll(value, cz - 1, 1))

    def y_before(value, field, x, t, slot):
        if t == 0:
            row = None if slot is None else halo_y[slot, pl.ds(x, 1), :]
        else:
            row = cur[field, x + 1, pl.ds(t * ROWS - 1, 1), :]
        row = 0.0 if row is None else jnp.broadcast_to(row, value.shape)
        return jnp.where(first_row, row, pltpu.roll(value, 1, 0))

    def y_after(value, field, x, t, slot):
        if t == tiles - 1:
            row = None if slot is None else halo_y[slot, pl.ds(x, 1), :]
        else:
            row = cur[field, x + 1, pl.ds(t * ROWS + ROWS, 1), :]
        row = 0.0 if row is None else jnp.broadcast_to(row, value.shape)
        return jnp.where(last_row, row, pltpu.roll(value, ROWS - 1, 0))

    def keep(step, field, x, rows, value):
        cur[field, x + 1, rows, :] = value
        if step == STEPS - 1:
            out[field, x, rows, :] = value

    def partials(step):
        for t in range(tiles):
            rows = pl.ds(t * ROWS, ROWS)
            sxx, sxy, sxz = tile(SXX, last, t), tile(SXY, last, t), tile(SXZ, last, t)
            part[step, 0, rows, :] = tile(VX, last, t) - (COURANT * coef[0, last, rows, :]) * (
                (sxy - y_before(sxy, SXY, last, t, None)) + (sxz - z_before(sxz)) - sxx)
        for t in range(tiles):
            rows = pl.ds(t * ROWS, ROWS)
            scaled = COURANT * coef[0, 0, rows, :]
            sxy, sxz, syz = tile(SXY, 0, t), tile(SXZ, 0, t), tile(SYZ, 0, t)
            syy, szz = tile(SYY, 0, t), tile(SZZ, 0, t)
            part[step, 1, rows, :] = tile(VY, 0, t) - scaled * (
                sxy + (y_after(syy, SYY, 0, t, None) - syy) + (syz - z_before(syz)))
            part[step, 2, rows, :] = tile(VZ, 0, t) - scaled * (
                sxz + (syz - y_before(syz, SYZ, 0, t, None)) + (z_after(szz) - szz))

    def velocity(step, which, x, want=(VX, VY, VZ)):
        slot = Y_SLOTS * step
        for t in which:
            rows = pl.ds(t * ROWS, ROWS)
            scaled = COURANT * coef[0, x, rows, :]
            sxy, sxz = tile(SXY, x, t), tile(SXZ, x, t)
            if VX in want:
                keep(step, VX, x, rows, tile(VX, x, t) - scaled * (
                    (tile(SXX, x + 1, t) - tile(SXX, x, t)) + (sxy - y_before(sxy, SXY, x, t, slot + Y_SXY))
                    + (sxz - z_before(sxz))))
            if VY in want:
                syy, syz, szz = tile(SYY, x, t), tile(SYZ, x, t), tile(SZZ, x, t)
                keep(step, VY, x, rows, tile(VY, x, t) - scaled * (
                    (sxy - tile(SXY, x - 1, t)) + (y_after(syy, SYY, x, t, slot + Y_SYY) - syy) + (syz - z_before(syz))))
                keep(step, VZ, x, rows, tile(VZ, x, t) - scaled * (
                    (sxz - tile(SXZ, x - 1, t)) + (syz - y_before(syz, SYZ, x, t, slot + Y_SYZ)) + (z_after(szz) - szz)))

    def complete(step):
        slot = Y_SLOTS * step
        for t in range(tiles):
            rows = pl.ds(t * ROWS, ROWS)

            def edge_row(value, row, at):
                return value + jnp.where(at, jnp.broadcast_to(row, (ROWS, cz)), 0.0)

            scaled = COURANT * coef[0, last, rows, :]
            more = halo_x[step, 3, rows, :]
            if t == 0:
                more = edge_row(more, -halo_y[slot + Y_SXY, pl.ds(last, 1), :], first_row)
            keep(step, VX, last, rows, part[step, 0, rows, :] - scaled * more)

            scaled = COURANT * coef[0, 0, rows, :]
            more = halo_x[step, 0, rows, :]
            if t == tiles - 1:
                more = edge_row(more, -halo_y[slot + Y_SYY, pl.ds(0, 1), :], last_row)
            keep(step, VY, 0, rows, part[step, 1, rows, :] + scaled * more)
            more = halo_x[step, 1, rows, :]
            if t == 0:
                more = edge_row(more, halo_y[slot + Y_SYZ, pl.ds(0, 1), :], first_row)
            keep(step, VZ, 0, rows, part[step, 2, rows, :] + scaled * more)

            more = tile(SXX, 0, t)
            if t == 0:
                more = edge_row(more, -corner[step, C_SXY], first_row)
            cur[VX, 0, rows, :] = halo_x[step, 2, rows, :] - (COURANT * halo_b[0, rows, :]) * more

            scaled = COURANT * halo_b[1, rows, :]
            more = tile(SXY, last, t)
            if t == tiles - 1:
                more = edge_row(more, -corner[step, C_SYY], last_row)
            cur[VY, cx + 1, rows, :] = halo_x[step, 4, rows, :] + scaled * more
            more = tile(SXZ, last, t)
            if t == 0:
                more = edge_row(more, corner[step, C_SYZ], first_row)
            cur[VZ, cx + 1, rows, :] = halo_x[step, 5, rows, :] + scaled * more

    def stress(step, which, x):
        slot = Y_SLOTS * step
        for t in which:
            rows = pl.ds(t * ROWS, ROWS)
            vx, vy, vz = tile(VX, x, t), tile(VY, x, t), tile(VZ, x, t)
            exx = vx - tile(VX, x - 1, t)
            eyy = vy - y_before(vy, VY, x, t, slot + Y_VY)
            ezz = vz - z_before(vz)
            exy = (y_after(vx, VX, x, t, slot + Y_VX) - vx) + (tile(VY, x + 1, t) - vy)
            exz = (z_after(vx) - vx) + (tile(VZ, x + 1, t) - vz)
            eyz = (z_after(vy) - vy) + (y_after(vz, VZ, x, t, slot + Y_VZ) - vz)
            both = (exx, eyy, ezz, exy, exz, eyz)
            for index, value in enumerate(both):
                strain[6 * step + index, x, rows, :] = value
            pull = (COURANT * coef[1, x, rows, :]) * (exx + eyy + ezz)
            mu = COURANT * coef[2, x, rows, :]
            for index, value in enumerate(both):
                change = pull + (2.0 * mu) * value if index < 3 else mu * value
                moved = tile(SXX + index, x, t) - change
                if step == STEPS - 1:
                    out[SXX + index, x, rows, :] = moved
                else:
                    cur[SXX + index, x + 1, rows, :] = moved

    def over(first, stop, body):
        def run(x, carry):
            body(x)
            return carry
        lax.fori_loop(first, stop, run, 0)

    def ends(body):
        def run(index, carry):
            body(index * (cx - 1))
            return carry
        lax.fori_loop(0, 2, run, 0)

    width = lanes
    per_x = cy * cz // (4 * segw)

    def source(row, chunk):
        offset = row * cz + chunk * width
        within = offset % (4 * segw)
        return offset // (4 * segw), within % segw, within // segw

    sub_w = lax.broadcasted_iota(jnp.int32, (ROWS, width), 0)

    def gradient(step, x):
        made = {}
        for t in range(tiles):
            for chunk in range(cz // width):
                rows = pl.ds(t * ROWS, ROWS)
                columns = pl.ds(chunk * width, width)
                plan = [source(t * ROWS + r, chunk) for r in range(ROWS)]
                shift = jnp.full((ROWS, width), 8 * plan[0][2], jnp.int32)
                for r in range(1, ROWS):
                    if plan[r][2] != plan[r - 1][2]:
                        shift = jnp.where(sub_w >= r, 8 * plan[r][2], shift)
                key = tuple(p[:2] for p in plan)
                distinct = list(dict.fromkeys(key))
                masks = []
                for item in distinct[1:]:
                    mask = None
                    for r in range(ROWS):
                        if key[r] == item:
                            mask = (sub_w == r) if mask is None else mask | (sub_w == r)
                    masks.append(mask)
                holders = {b: inv[0, x * per_x + b] for b in dict.fromkeys(k[0] for k in key)}
                blocks = [k[0] for k in key]

                def stored(c):
                    if (key, c) not in made:
                        word = None
                        for position, (block, start) in enumerate(distinct):
                            piece = jnp.broadcast_to(
                                words[step][holders[block], c - per_step * step, pl.ds(start // lanes, 1), :], (ROWS, width))
                            word = piece if word is None else jnp.where(masks[position - 1], piece, word)
                        made[key, c] = word ^ jnp.int32(-2147483648)
                    byte = (lax.shift_right_logical(made[key, c], shift) & 255) - 128
                    factor = None
                    for r in range(ROWS):
                        if r == 0:
                            factor = factor_s[holders[blocks[0]], 0, c]
                        elif blocks[r] != blocks[r - 1]:
                            factor = jnp.where(sub_w >= r, factor_s[holders[blocks[r]], 0, c], factor)
                    return byte.astype(jnp.float32) * factor

                e = [strain[6 * step + index, x, rows, columns] for index in range(6)]
                f = [stored(6 * step + index) for index in range(6)]
                grad_lambda = (e[0] + e[1] + e[2]) * (f[0] + f[1] + f[2])
                grad_mu = 2.0 * (e[0] * f[0] + e[1] * f[1] + e[2] * f[2])
                grad_mu = grad_mu + e[3] * f[3] + e[4] * f[4] + e[5] * f[5]
                if step > 0:
                    grad_lambda = grads[0, x, rows, columns] + grad_lambda
                    grad_mu = grads[1, x, rows, columns] + grad_mu
                grads[0, x, rows, columns] = grad_lambda
                grads[1, x, rows, columns] = grad_mu

    for way_x, way_y, first, fields in CORNERS:
        @pl.when(jnp.logical_not(both_edges(-way_x, -way_y)))
        def _():
            for step in range(STEPS):
                for offset in range(len(fields)):
                    corner[step, first + offset] = jnp.zeros((1, cz), jnp.float32)

    for way in (-1, 1):
        @pl.when(jnp.logical_not(edge(way, "gx")))
        def _():
            zero = jnp.zeros((ROWS, cz), jnp.float32)
            for t in range(tiles):
                rows = pl.ds(t * ROWS, ROWS)
                halo_b[0 if way < 0 else 1, rows, :] = zero
                for step in range(STEPS):
                    for slot in (0, 1, 2) if way < 0 else (3, 4, 5):
                        halo_x[step, slot, rows, :] = zero

        @pl.when(jnp.logical_not(edge(way, "gy")))
        def _():
            for step in range(STEPS):
                for start, count, sent in STRESS_Y + SPEED_Y:
                    if sent == -way:
                        for offset in range(count):
                            halo_y[Y_SLOTS * step + start + offset] = jnp.zeros((cx, cz), jnp.float32)
            halo_y[Y_SLOTS * STEPS + (0 if way > 0 else 1)] = jnp.zeros((cx, cz), jnp.float32)

    outer = (0, tiles - 1) if tiles > 1 else (0,)
    inner = range(1, tiles - 1)
    every = range(tiles)
    waited = set()

    def need(*which):
        for index in which:
            if index not in waited:
                loads[index].wait()
                waited.add(index)

    need(*range(12))
    partials(0)

    beside_x = jnp.minimum(me_x, 1) + jnp.minimum(n_x - 1 - me_x, 1)
    beside_y = jnp.minimum(me_y, 1) + jnp.minimum(n_y - 1 - me_y, 1)
    pl.semaphore_wait(barrier, n_x - 1 + beside_y + beside_x * beside_y)

    send_stress_y(0)
    send_corners(0)
    send_buoy_y()
    x_start(0, DOWN_B, UP_B, DOWN_S, UP_S, DOWN_V, UP_V)
    send_relays()
    send_words(0, near)

    load_scales.wait()
    load_perm.wait()
    square = 128
    sub_q = lax.broadcasted_iota(jnp.int32, (square, square), 0)
    lane_q = lax.broadcasted_iota(jnp.int32, (square, square), 1)
    table[...] = jnp.zeros((16, square), jnp.float32)
    for c in range(comp):
        table[pl.ds(c, 1), pl.ds(0, n_x)] = scale_v[c]
    by_owner = jnp.transpose(jnp.concatenate([table[...], jnp.zeros((square - 16, square), jnp.float32)], axis=0))
    for owner in range(n_x):
        factor_send[owner] = by_owner[owner:owner + 1, :comp]
    inv_v[...] = jnp.full((1, square), -1, jnp.int32)
    inv_v[pl.ds(0, 1), pl.ds(0, n_x)] = perm_v[...]
    by_holder = jnp.transpose(jnp.broadcast_to(inv_v[...], (square, square)))
    inv_v[...] = jnp.max(jnp.where(by_holder == lane_q, sub_q, 0), axis=0, keepdims=True)
    inverse = pltpu.make_async_copy(inv_v, inv, loc_sem.at[0])
    inverse.start()
    own_factor = pltpu.make_async_copy(factor_send.at[me_x], factors.at[me_x], loc_sem.at[1])
    own_factor.start()

    def send_factors():
        for distance in near + far:
            factor_copy(distance).start()

    for step in range(STEPS):
        if step > 0:
            partials(step)
            send_stress_y(step)
            send_corners(step)
            x_start(step, DOWN_S, UP_S, DOWN_V, UP_V)
        if step == 1:
            pass
            pass
        velocity(step, inner, 0, (VX,))
        velocity(step, inner, last, (VY, VZ))
        over(1, last, functools.partial(velocity, step, inner))
        receive_y(step, STRESS_Y)
        velocity(step, outer, 0, (VX,))
        velocity(step, outer, last, (VY, VZ))
        over(1, last, functools.partial(velocity, step, outer))
        send_speed_y(step)
        if step == 0:
            send_factors()
            pass
            words_of([(0, far[16:])], [(0, far)])
        else:
            pass_relays()
            words_of([(1, far), (1, near)], [(1, far), (1, near)])
        over(1, last, functools.partial(stress, step, inner))
        if step == 1:
            own_factor.wait()
            for distance in near + far:
                factor_copy(distance).wait()
            to_scalar = pltpu.make_async_copy(factors, factor_s, loc_sem.at[1])
            to_scalar.start()
        x_wait(step, "recv", DOWN_S, DOWN_V, UP_S, UP_V)
        if step == 0:
            receive_y(STEPS, BUOY_Y)
            x_wait(0, "recv", DOWN_B, UP_B)
        receive_corners(step)
        complete(step)
        receive_y(step, SPEED_Y)
        if step == 0:
            pass
            pass
        fix_rows(step)
        ends(functools.partial(stress, step, every))
        over(1, last, functools.partial(stress, step, outer))
    to_scalar.wait()
    inverse.wait()
    receive_words(0)
    over(0, cx, functools.partial(gradient, 0))
    receive_words(STEPS - 1)
    over(0, cx, functools.partial(gradient, STEPS - 1))

    finish_relays()
    for step in range(STEPS):
        x_wait(step, "send", DOWN_S, DOWN_V, UP_S, UP_V)
        for message in STRESS_Y + SPEED_Y:
            @pl.when(edge(message[2], "gy"))
            def _():
                y_copy(step, message).wait_send()
        for which, (way_x, way_y, _, _) in enumerate(CORNERS):
            @pl.when(both_edges(way_x, way_y))
            def _():
                corner_copy(step, which).wait_send()
    for message in BUOY_Y:
        @pl.when(edge(message[2], "gy"))
        def _():
            y_copy(STEPS, message).wait_send()
    x_wait(0, "send", DOWN_B, UP_B)


def on_device(n_x, n_y, adjoint, buoyancy, lame_lambda, shear_mu, packed, scales, perm):
    fields, cx, cy, cz = adjoint.shape
    comp, segw = packed.shape[3:]
    lanes = min(128, segw)
    packed = packed.reshape(n_x, comp, segw // lanes, lanes)
    scales = jnp.transpose(scales, (0, 3, 2, 1)).reshape(comp, 1, n_x)
    halos = Y_SLOTS * STEPS + 2
    dma = pltpu.SemaphoreType.DMA
    f32, i32 = jnp.float32, jnp.int32
    return pl.pallas_call(
        functools.partial(kernel, n_x, n_y),
        out_shape=(pltpu.VMEM(adjoint.shape, f32), pltpu.VMEM((2, cx, cy, cz), f32)),
        in_specs=[pl.BlockSpec(memory_space=pltpu.HBM)] * 7,
        out_specs=(pl.BlockSpec(memory_space=pltpu.VMEM),) * 2,
        scratch_shapes=[
            pltpu.VMEM((fields, cx + 2, cy, cz), f32),
            pltpu.VMEM((3, cx, cy, cz), f32),
            pltpu.VMEM((comp, cx, cy, cz), f32),
            pltpu.VMEM((STEPS, 6, cy, cz), f32),
            pltpu.VMEM((2, cy, cz), f32),
            pltpu.VMEM((STEPS, 3, cy, cz), f32),
            pltpu.VMEM((STEPS, 5, 1, cz), f32),
            pltpu.VMEM((STEPS, 5, 1, cz), f32),
            pltpu.VMEM((halos, cx, cz), f32),
            pltpu.VMEM((halos, cx, cz), f32),
            pltpu.VMEM((max(16, 1), comp // STEPS, segw // lanes, lanes), i32),
            pltpu.VMEM((16, 128), f32),
            pltpu.VMEM((comp, 1, n_x), f32),
            pltpu.VMEM((n_x, 1, comp), f32),
            pltpu.VMEM((n_x, 1, comp), f32),
            pltpu.SMEM((n_x, 1, comp), f32),
            pltpu.VMEM((1, n_x), i32),
            pltpu.VMEM((1, 128), i32),
            pltpu.SMEM((1, 128), i32),
            dma((12,)), dma((STEPS, 6)), dma((STEPS, 6)), dma((STEPS, 4)), dma((STEPS, 4)), dma((max(16, 1),)), dma((max(16, 1),)), dma((halos,)), dma((halos,)),
            dma((n_x, STEPS)), dma((n_x, STEPS)), dma((n_x,)), dma((n_x,)), dma((2 + STEPS,)),
        ] + [pltpu.VMEM((n_x, comp // STEPS, segw // lanes, lanes), i32)] * STEPS,
        compiler_params=pltpu.CompilerParams(collective_id=0, has_side_effects=True,
                                             vmem_limit_bytes=64000000),
    )(adjoint, buoyancy, lame_lambda, shear_mu, packed, scales, perm)


def solution(mesh):
    return jax.shard_map(
        functools.partial(on_device, mesh.shape["gx"], mesh.shape["gy"]),
        mesh=mesh,
        in_specs=(
            P(None, "gx", "gy", None),
            P("gx", "gy", None),
            P("gx", "gy", None),
            P("gx", "gy", None),
            P("gx", None, "gy", None, None),
            P("gx", None, "gy", None),
            P("gx", None),
        ),
        out_specs=(P(None, "gx", "gy", None), P(None, "gx", "gy", None)),
        check_vma=False,
    )
```

```python
import functools

import jax
import jax.numpy as jnp
from jax import lax
from jax.experimental import pallas as pl
from jax.experimental.pallas import tpu as pltpu
from jax.sharding import PartitionSpec as P

MESH = pl.DeviceIdType.MESH
STEPS = 2
COURANT = 0.15
ROWS = 8
ZBIT = 8
PAIR = 2

VX, VY, VZ, SXX, SYY, SZZ, SXY, SXZ, SYZ = range(9)

DOWN_S, DOWN_V, DOWN_B, UP_S, UP_V, UP_B = range(6)
Y_SLOTS = 6
Y_SYY, Y_SXY, Y_SYZ, Y_VX, Y_VZ, Y_VY = range(Y_SLOTS)
STRESS_Y = ((Y_SYY, 1, -1), (Y_SXY, 2, 1))
SPEED_Y = ((Y_VX, 2, -1), (Y_VY, 1, 1))
BUOY_Y = ((0, 1, -1), (1, 1, 1))
C_SXY, C_SXZ, C_SYY, C_SXX, C_SYZ = range(5)
CORNERS = ((1, 1, C_SXY, ((SXY, 1, 1),)), (1, -1, C_SXZ, ((SXZ, 1, 0),)),
           (-1, -1, C_SYY, ((SYY, 0, 0), (SXX, 0, 0))), (-1, 1, C_SYZ, ((SYZ, 0, 1),)))


def partner(me, distance, count):
    if count & (count - 1):
        return lax.rem(me + distance, count)
    result, bit = me, 1
    while bit < count:
        if distance & bit:
            result = result + bit - 2 * bit * ((me // bit) % 2)
        bit *= 2
    return result


def kernel(n_x, n_y, adj, buoy, lam, shear, packed, scales, perm, out, grads,
           cur, coef, strain, halo_x, halo_b, part, corner, corner_send, halo_y, send_y,
           relay, table, scale_v, factor_send, factors, factor_s, perm_v, inv_v, inv,
           in_sem, xs_sem, xr_sem, cs_sem, cr_sem, rs_sem, rr_sem, ys_sem, yr_sem, ws_sem, wr_sem, fs_sem, fr_sem, loc_sem, *words):
    cx, cy, cz = buoy.shape
    comp = packed.shape[1]
    per_step = comp // STEPS
    lanes = packed.shape[3]
    segw = packed.shape[2] * lanes
    tiles = cy // ROWS
    last = cx - 1
    me_x, me_y = lax.axis_index("gx"), lax.axis_index("gy")

    barrier = pltpu.get_barrier_semaphore()
    for distance in range(1, n_x):
        pl.semaphore_signal(barrier, inc=1, device_id={"gx": partner(me_x, distance, n_x)}, device_id_type=MESH)

    def edge(way, axis):
        me, count = (me_x, n_x) if axis == "gx" else (me_y, n_y)
        return (me > 0) if way < 0 else (me < count - 1)

    for way in (-1, 1):
        @pl.when(edge(way, "gy"))
        def _():
            pl.semaphore_signal(barrier, inc=1, device_id={"gy": me_y + way}, device_id_type=MESH)

        for way_x in (-1, 1):
            @pl.when(edge(way, "gy") & edge(way_x, "gx"))
            def _():
                pl.semaphore_signal(barrier, inc=1, device_id={"gx": me_x + way_x, "gy": me_y + way},
                                    device_id_type=MESH)

    loads = {}
    for index in (SXX, SXY, SXZ, SYY, SYZ, SZZ, VX, VY, VZ):
        loads[index] = pltpu.make_async_copy(adj.at[index], cur.at[index, pl.ds(1, cx)], in_sem.at[index])
    for index, ref in enumerate((buoy, lam, shear)):
        loads[9 + index] = pltpu.make_async_copy(ref, coef.at[index], in_sem.at[9 + index])
    load_perm = pltpu.make_async_copy(perm, perm_v, loc_sem.at[0])
    load_scales = pltpu.make_async_copy(scales, scale_v, loc_sem.at[1])
    own_words = [pltpu.make_async_copy(packed.at[me_x, pl.ds(step * per_step, per_step)], words[step].at[me_x],
                                       loc_sem.at[2 + step]) for step in range(STEPS)]
    for index in (9, SXY, SXZ, SYZ, SXX, SYY, SZZ, VX, VY, VZ, 10, 11):
        loads[index].start()
    load_perm.start()
    load_scales.start()
    for copy in own_words:
        copy.start()

    def x_copy(step, kind):
        way = 1 if kind < UP_S else -1
        if kind == DOWN_S:
            fields = pl.ds(SXY, 2)
            src = adj.at[fields, last] if step == 0 else cur.at[fields, cx]
            dst = halo_x.at[step, pl.ds(0, 2)]
        elif kind == DOWN_V:
            src, dst = part.at[step, pl.ds(0, 1)], halo_x.at[step, pl.ds(2, 1)]
        elif kind == DOWN_B:
            src, dst = buoy.at[last], halo_b.at[0]
        elif kind == UP_S:
            src, dst = (adj.at[SXX, 0] if step == 0 else cur.at[SXX, 1]), halo_x.at[step, 3]
        elif kind == UP_V:
            src, dst = part.at[step, pl.ds(1, 2)], halo_x.at[step, pl.ds(4, 2)]
        else:
            src, dst = buoy.at[0], halo_b.at[1]
        return way, pltpu.make_async_remote_copy(
            src_ref=src, dst_ref=dst, send_sem=xs_sem.at[step, kind], recv_sem=xr_sem.at[step, kind],
            device_id={"gx": me_x + way}, device_id_type=MESH)

    def x_start(step, *kinds):
        for kinds_way, way in ((kinds[:], 1), (kinds[:], -1)):
            mine = [k for k in kinds_way if (k < UP_S) == (way == 1)]
            if mine:
                @pl.when(edge(way, "gx"))
                def _():
                    for kind in mine:
                        x_copy(step, kind)[1].start()

    def x_wait(step, what, *kinds):
        for way in (1, -1):
            mine = [k for k in kinds if (k < UP_S) == (way == 1)]
            if mine:
                @pl.when(edge(-way if what == "recv" else way, "gx"))
                def _():
                    for kind in mine:
                        copy = x_copy(step, kind)[1]
                        if what == "recv":
                            copy.wait_recv()
                        else:
                            copy.wait_send()

    def y_copy(step, message):
        start, count, way = message
        slot = Y_SLOTS * step + start
        return pltpu.make_async_remote_copy(
            src_ref=send_y.at[pl.ds(slot, count)], dst_ref=halo_y.at[pl.ds(slot, count)],
            send_sem=ys_sem.at[slot], recv_sem=yr_sem.at[slot],
            device_id={"gy": me_y + way}, device_id_type=MESH)

    def y_start(step, message):
        y_copy(step, message).start()

    def receive_y(step, messages):
        for message in messages:
            @pl.when(edge(-message[2], "gy"))
            def _():
                y_copy(step, message).wait_recv()

    def row_of(field, x, row):
        return cur[field, 1 + x, pl.ds(row, 1), :]

    def send_buoy_y():
        @pl.when(edge(-1, "gy"))
        def _():
            send_y[Y_SLOTS * STEPS, pl.ds(0, 1), :] = coef[0, last, pl.ds(0, 1), :]
            send_y[Y_SLOTS * STEPS, pl.ds(1, 1), :] = coef[0, 0, pl.ds(0, 1), :]
            y_start(STEPS, BUOY_Y[0])

        @pl.when(edge(1, "gy"))
        def _():
            send_y[Y_SLOTS * STEPS + 1, pl.ds(0, 1), :] = coef[0, 0, pl.ds(cy - 1, 1), :]
            y_start(STEPS, BUOY_Y[1])

    def send_stress_y(step):
        slot = Y_SLOTS * step

        @pl.when(edge(-1, "gy"))
        def _():
            for x in range(cx):
                send_y[slot + Y_SYY, pl.ds(x, 1), :] = row_of(SYY, x, 0)
            y_start(step, STRESS_Y[0])

        @pl.when(edge(1, "gy"))
        def _():
            for x in range(cx):
                send_y[slot + Y_SXY, pl.ds(x, 1), :] = row_of(SXY, x, cy - 1)
                send_y[slot + Y_SYZ, pl.ds(x, 1), :] = row_of(SYZ, x, cy - 1)
            y_start(step, STRESS_Y[1])

    def send_speed_y(step):
        slot = Y_SLOTS * step

        @pl.when(edge(-1, "gy"))
        def _():
            first = pl.ds(0, 1)
            for x in range(last):
                send_y[slot + Y_VX, pl.ds(x, 1), :] = row_of(VX, x, 0)
                send_y[slot + Y_VZ, pl.ds(x + 1, 1), :] = row_of(VZ, x + 1, 0)
            send_y[slot + Y_VX, pl.ds(last, 1), :] = part[step, 0, first, :] + (
                COURANT * coef[0, last, first, :]) * halo_y[slot + Y_SXY, pl.ds(last, 1), :]
            send_y[slot + Y_VZ, pl.ds(0, 1), :] = part[step, 2, first, :] + (
                COURANT * coef[0, 0, first, :]) * halo_y[slot + Y_SYZ, pl.ds(0, 1), :]
            y_start(step, SPEED_Y[0])

        @pl.when(edge(1, "gy"))
        def _():
            end = pl.ds(cy - 1, 1)
            for x in range(1, cx):
                send_y[slot + Y_VY, pl.ds(x, 1), :] = row_of(VY, x, cy - 1)
            send_y[slot + Y_VY, pl.ds(0, 1), :] = part[step, 1, end, :] - (
                COURANT * coef[0, 0, end, :]) * halo_y[slot + Y_SYY, pl.ds(0, 1), :]
            y_start(step, SPEED_Y[1])

    def fix_rows(step):
        slot, extra = Y_SLOTS * step, Y_SLOTS * STEPS
        one, end = pl.ds(0, 1), pl.ds(last, 1)
        halo_y[slot + Y_VX, end, :] = halo_y[slot + Y_VX, end, :] - (
            COURANT * halo_y[extra, one, :]) * corner[step, C_SXX]
        halo_y[slot + Y_VZ, one, :] = halo_y[slot + Y_VZ, one, :] + (
            COURANT * halo_y[extra, pl.ds(1, 1), :]) * corner[step, C_SXZ]
        halo_y[slot + Y_VY, one, :] = halo_y[slot + Y_VY, one, :] + (
            COURANT * halo_y[extra + 1, one, :]) * corner[step, C_SXY]

    def both_edges(way_x, way_y):
        return edge(way_x, "gx") & edge(way_y, "gy")

    def corner_copy(step, which):
        way_x, way_y, first, fields = CORNERS[which]
        slots = pl.ds(first, len(fields))
        return pltpu.make_async_remote_copy(
            src_ref=corner_send.at[step, slots], dst_ref=corner.at[step, slots],
            send_sem=cs_sem.at[step, which], recv_sem=cr_sem.at[step, which],
            device_id={"gx": me_x + way_x, "gy": me_y + way_y}, device_id_type=MESH)

    def send_corners(step):
        for which, (way_x, way_y, first, fields) in enumerate(CORNERS):
            @pl.when(both_edges(way_x, way_y))
            def _():
                for offset, (field, layer, row) in enumerate(fields):
                    corner_send[step, first + offset] = row_of(field, layer * last, row * (cy - 1))
                corner_copy(step, which).start()

    def receive_corners(step):
        for which, (way_x, way_y, first, fields) in enumerate(CORNERS):
            @pl.when(both_edges(-way_x, -way_y))
            def _():
                corner_copy(step, which).wait_recv()

    def word_copy(distance, step):
        to = partner(me_x, distance, n_x)
        stored = pl.ds(step * per_step, per_step)
        return pltpu.make_async_remote_copy(
            src_ref=packed.at[to, stored], dst_ref=words[step].at[me_x], send_sem=ws_sem.at[distance, step],
            recv_sem=wr_sem.at[distance, step], device_id={"gx": to}, device_id_type=MESH)

    def factor_copy(distance):
        to = partner(me_x, distance, n_x)
        return pltpu.make_async_remote_copy(
            src_ref=factor_send.at[to], dst_ref=factors.at[me_x], send_sem=fs_sem.at[distance],
            recv_sem=fr_sem.at[distance], device_id={"gx": to}, device_id_type=MESH)

    far = [d for d in range(1, n_x) if d & ZBIT]
    near = [d for d in range(1, n_x) if not d & ZBIT]

    place = me_x % 8
    slow = (place == 0) | (place == 7)
    quick = jnp.logical_not(slow)
    beside = (place == 1) | (place == 6)
    relays = (place == 2) | (place == 5)
    inside = (place >= 2) & (place <= 5)
    relayed = [(0, d) for d in far]

    def relay_in(index):
        step, distance = relayed[index]
        to = partner(me_x, distance, n_x)
        return pltpu.make_async_remote_copy(
            src_ref=packed.at[to, pl.ds(step * per_step, per_step)], dst_ref=relay.at[index],
            send_sem=ws_sem.at[distance, step], recv_sem=rr_sem.at[index],
            device_id={"gx": partner(me_x, PAIR, n_x)}, device_id_type=MESH)

    def relay_out(index):
        step, distance = relayed[index]
        return pltpu.make_async_remote_copy(
            src_ref=relay.at[index], dst_ref=words[step].at[partner(me_x, PAIR, n_x)],
            send_sem=rs_sem.at[index], recv_sem=wr_sem.at[distance, step],
            device_id={"gx": partner(me_x, distance ^ PAIR, n_x)}, device_id_type=MESH)

    def send_relays():
        @pl.when(slow)
        def _():
            for index in range(len(relayed)):
                relay_in(index).start()

    def pass_relays():
        @pl.when(relays)
        def _():
            for index in range(len(relayed)):
                relay_in(index).wait_recv()
                relay_out(index).start()

    def finish_relays():
        @pl.when(relays)
        def _():
            for index in range(len(relayed)):
                relay_out(index).wait_send()

    def words_of(where, *which):
        @pl.when(where)
        def _():
            for step, distances in which:
                send_words(step, distances)

    def send_words(step, distances):
        for distance in distances:
            word_copy(distance, step).start()

    def receive_words(step):
        own_words[step].wait()
        for distance in near + far:
            word_copy(distance, step).wait()

    sub = lax.broadcasted_iota(jnp.int32, (ROWS, cz), 0)
    lane = lax.broadcasted_iota(jnp.int32, (ROWS, cz), 1)
    first_row, last_row = sub == 0, sub == ROWS - 1
    first_lane, last_lane = lane == 0, lane == cz - 1

    def tile(field, x, t):
        return cur[field, x + 1, pl.ds(t * ROWS, ROWS), :]

    def z_before(value):
        return jnp.where(first_lane, 0.0, pltpu.roll(value, 1, 1))

    def z_after(value):
        return jnp.where(last_lane, 0.0, pltpu.roll(value, cz - 1, 1))

    def y_before(value, field, x, t, slot):
        if t == 0:
            row = None if slot is None else halo_y[slot, pl.ds(x, 1), :]
        else:
            row = cur[field, x + 1, pl.ds(t * ROWS - 1, 1), :]
        row = 0.0 if row is None else jnp.broadcast_to(row, value.shape)
        return jnp.where(first_row, row, pltpu.roll(value, 1, 0))

    def y_after(value, field, x, t, slot):
        if t == tiles - 1:
            row = None if slot is None else halo_y[slot, pl.ds(x, 1), :]
        else:
            row = cur[field, x + 1, pl.ds(t * ROWS + ROWS, 1), :]
        row = 0.0 if row is None else jnp.broadcast_to(row, value.shape)
        return jnp.where(last_row, row, pltpu.roll(value, ROWS - 1, 0))

    def keep(step, field, x, rows, value):
        cur[field, x + 1, rows, :] = value
        if step == STEPS - 1:
            out[field, x, rows, :] = value

    def partials(step):
        for t in range(tiles):
            rows = pl.ds(t * ROWS, ROWS)
            sxx, sxy, sxz = tile(SXX, last, t), tile(SXY, last, t), tile(SXZ, last, t)
            part[step, 0, rows, :] = tile(VX, last, t) - (COURANT * coef[0, last, rows, :]) * (
                (sxy - y_before(sxy, SXY, last, t, None)) + (sxz - z_before(sxz)) - sxx)
        for t in range(tiles):
            rows = pl.ds(t * ROWS, ROWS)
            scaled = COURANT * coef[0, 0, rows, :]
            sxy, sxz, syz = tile(SXY, 0, t), tile(SXZ, 0, t), tile(SYZ, 0, t)
            syy, szz = tile(SYY, 0, t), tile(SZZ, 0, t)
            part[step, 1, rows, :] = tile(VY, 0, t) - scaled * (
                sxy + (y_after(syy, SYY, 0, t, None) - syy) + (syz - z_before(syz)))
            part[step, 2, rows, :] = tile(VZ, 0, t) - scaled * (
                sxz + (syz - y_before(syz, SYZ, 0, t, None)) + (z_after(szz) - szz))

    def velocity(step, which, x, want=(VX, VY, VZ)):
        slot = Y_SLOTS * step
        for t in which:
            rows = pl.ds(t * ROWS, ROWS)
            scaled = COURANT * coef[0, x, rows, :]
            sxy, sxz = tile(SXY, x, t), tile(SXZ, x, t)
            if VX in want:
                keep(step, VX, x, rows, tile(VX, x, t) - scaled * (
                    (tile(SXX, x + 1, t) - tile(SXX, x, t)) + (sxy - y_before(sxy, SXY, x, t, slot + Y_SXY))
                    + (sxz - z_before(sxz))))
            if VY in want:
                syy, syz, szz = tile(SYY, x, t), tile(SYZ, x, t), tile(SZZ, x, t)
                keep(step, VY, x, rows, tile(VY, x, t) - scaled * (
                    (sxy - tile(SXY, x - 1, t)) + (y_after(syy, SYY, x, t, slot + Y_SYY) - syy) + (syz - z_before(syz))))
                keep(step, VZ, x, rows, tile(VZ, x, t) - scaled * (
                    (sxz - tile(SXZ, x - 1, t)) + (syz - y_before(syz, SYZ, x, t, slot + Y_SYZ)) + (z_after(szz) - szz)))

    def complete(step):
        slot = Y_SLOTS * step
        for t in range(tiles):
            rows = pl.ds(t * ROWS, ROWS)

            def edge_row(value, row, at):
                return value + jnp.where(at, jnp.broadcast_to(row, (ROWS, cz)), 0.0)

            scaled = COURANT * coef[0, last, rows, :]
            more = halo_x[step, 3, rows, :]
            if t == 0:
                more = edge_row(more, -halo_y[slot + Y_SXY, pl.ds(last, 1), :], first_row)
            keep(step, VX, last, rows, part[step, 0, rows, :] - scaled * more)

            scaled = COURANT * coef[0, 0, rows, :]
            more = halo_x[step, 0, rows, :]
            if t == tiles - 1:
                more = edge_row(more, -halo_y[slot + Y_SYY, pl.ds(0, 1), :], last_row)
            keep(step, VY, 0, rows, part[step, 1, rows, :] + scaled * more)
            more = halo_x[step, 1, rows, :]
            if t == 0:
                more = edge_row(more, halo_y[slot + Y_SYZ, pl.ds(0, 1), :], first_row)
            keep(step, VZ, 0, rows, part[step, 2, rows, :] + scaled * more)

            more = tile(SXX, 0, t)
            if t == 0:
                more = edge_row(more, -corner[step, C_SXY], first_row)
            cur[VX, 0, rows, :] = halo_x[step, 2, rows, :] - (COURANT * halo_b[0, rows, :]) * more

            scaled = COURANT * halo_b[1, rows, :]
            more = tile(SXY, last, t)
            if t == tiles - 1:
                more = edge_row(more, -corner[step, C_SYY], last_row)
            cur[VY, cx + 1, rows, :] = halo_x[step, 4, rows, :] + scaled * more
            more = tile(SXZ, last, t)
            if t == 0:
                more = edge_row(more, corner[step, C_SYZ], first_row)
            cur[VZ, cx + 1, rows, :] = halo_x[step, 5, rows, :] + scaled * more

    def stress(step, which, x):
        slot = Y_SLOTS * step
        for t in which:
            rows = pl.ds(t * ROWS, ROWS)
            vx, vy, vz = tile(VX, x, t), tile(VY, x, t), tile(VZ, x, t)
            exx = vx - tile(VX, x - 1, t)
            eyy = vy - y_before(vy, VY, x, t, slot + Y_VY)
            ezz = vz - z_before(vz)
            exy = (y_after(vx, VX, x, t, slot + Y_VX) - vx) + (tile(VY, x + 1, t) - vy)
            exz = (z_after(vx) - vx) + (tile(VZ, x + 1, t) - vz)
            eyz = (z_after(vy) - vy) + (y_after(vz, VZ, x, t, slot + Y_VZ) - vz)
            both = (exx, eyy, ezz, exy, exz, eyz)
            for index, value in enumerate(both):
                strain[6 * step + index, x, rows, :] = value
            pull = (COURANT * coef[1, x, rows, :]) * (exx + eyy + ezz)
            mu = COURANT * coef[2, x, rows, :]
            for index, value in enumerate(both):
                change = pull + (2.0 * mu) * value if index < 3 else mu * value
                moved = tile(SXX + index, x, t) - change
                if step == STEPS - 1:
                    out[SXX + index, x, rows, :] = moved
                else:
                    cur[SXX + index, x + 1, rows, :] = moved

    def over(first, stop, body):
        def run(x, carry):
            body(x)
            return carry
        lax.fori_loop(first, stop, run, 0)

    def ends(body):
        def run(index, carry):
            body(index * (cx - 1))
            return carry
        lax.fori_loop(0, 2, run, 0)

    width = lanes
    per_x = cy * cz // (4 * segw)

    def source(row, chunk):
        offset = row * cz + chunk * width
        within = offset % (4 * segw)
        return offset // (4 * segw), within % segw, within // segw

    sub_w = lax.broadcasted_iota(jnp.int32, (ROWS, width), 0)

    def gradient(step, x):
        made = {}
        for t in range(tiles):
            for chunk in range(cz // width):
                rows = pl.ds(t * ROWS, ROWS)
                columns = pl.ds(chunk * width, width)
                plan = [source(t * ROWS + r, chunk) for r in range(ROWS)]
                shift = jnp.full((ROWS, width), 8 * plan[0][2], jnp.int32)
                for r in range(1, ROWS):
                    if plan[r][2] != plan[r - 1][2]:
                        shift = jnp.where(sub_w >= r, 8 * plan[r][2], shift)
                key = tuple(p[:2] for p in plan)
                distinct = list(dict.fromkeys(key))
                masks = []
                for item in distinct[1:]:
                    mask = None
                    for r in range(ROWS):
                        if key[r] == item:
                            mask = (sub_w == r) if mask is None else mask | (sub_w == r)
                    masks.append(mask)
                holders = {b: inv[0, x * per_x + b] for b in dict.fromkeys(k[0] for k in key)}
                blocks = [k[0] for k in key]

                def stored(c):
                    if (key, c) not in made:
                        word = None
                        for position, (block, start) in enumerate(distinct):
                            piece = jnp.broadcast_to(
                                words[step][holders[block], c - per_step * step, pl.ds(start // lanes, 1), :], (ROWS, width))
                            word = piece if word is None else jnp.where(masks[position - 1], piece, word)
                        made[key, c] = word ^ jnp.int32(-2147483648)
                    byte = (lax.shift_right_logical(made[key, c], shift) & 255) - 128
                    factor = None
                    for r in range(ROWS):
                        if r == 0:
                            factor = factor_s[holders[blocks[0]], 0, c]
                        elif blocks[r] != blocks[r - 1]:
                            factor = jnp.where(sub_w >= r, factor_s[holders[blocks[r]], 0, c], factor)
                    return byte.astype(jnp.float32) * factor

                e = [strain[6 * step + index, x, rows, columns] for index in range(6)]
                f = [stored(6 * step + index) for index in range(6)]
                grad_lambda = (e[0] + e[1] + e[2]) * (f[0] + f[1] + f[2])
                grad_mu = 2.0 * (e[0] * f[0] + e[1] * f[1] + e[2] * f[2])
                grad_mu = grad_mu + e[3] * f[3] + e[4] * f[4] + e[5] * f[5]
                if step > 0:
                    grad_lambda = grads[0, x, rows, columns] + grad_lambda
                    grad_mu = grads[1, x, rows, columns] + grad_mu
                grads[0, x, rows, columns] = grad_lambda
                grads[1, x, rows, columns] = grad_mu

    for way_x, way_y, first, fields in CORNERS:
        @pl.when(jnp.logical_not(both_edges(-way_x, -way_y)))
        def _():
            for step in range(STEPS):
                for offset in range(len(fields)):
                    corner[step, first + offset] = jnp.zeros((1, cz), jnp.float32)

    for way in (-1, 1):
        @pl.when(jnp.logical_not(edge(way, "gx")))
        def _():
            zero = jnp.zeros((ROWS, cz), jnp.float32)
            for t in range(tiles):
                rows = pl.ds(t * ROWS, ROWS)
                halo_b[0 if way < 0 else 1, rows, :] = zero
                for step in range(STEPS):
                    for slot in (0, 1, 2) if way < 0 else (3, 4, 5):
                        halo_x[step, slot, rows, :] = zero

        @pl.when(jnp.logical_not(edge(way, "gy")))
        def _():
            for step in range(STEPS):
                for start, count, sent in STRESS_Y + SPEED_Y:
                    if sent == -way:
                        for offset in range(count):
                            halo_y[Y_SLOTS * step + start + offset] = jnp.zeros((cx, cz), jnp.float32)
            halo_y[Y_SLOTS * STEPS + (0 if way > 0 else 1)] = jnp.zeros((cx, cz), jnp.float32)

    outer = (0, tiles - 1) if tiles > 1 else (0,)
    inner = range(1, tiles - 1)
    every = range(tiles)
    waited = set()

    def need(*which):
        for index in which:
            if index not in waited:
                loads[index].wait()
                waited.add(index)

    need(*range(12))
    partials(0)

    beside_x = jnp.minimum(me_x, 1) + jnp.minimum(n_x - 1 - me_x, 1)
    beside_y = jnp.minimum(me_y, 1) + jnp.minimum(n_y - 1 - me_y, 1)
    pl.semaphore_wait(barrier, n_x - 1 + beside_y + beside_x * beside_y)

    send_stress_y(0)
    send_corners(0)
    send_buoy_y()
    x_start(0, DOWN_B, UP_B, DOWN_S, UP_S, DOWN_V, UP_V)
    send_relays()
    send_words(0, near)

    load_scales.wait()
    load_perm.wait()
    square = 128
    sub_q = lax.broadcasted_iota(jnp.int32, (square, square), 0)
    lane_q = lax.broadcasted_iota(jnp.int32, (square, square), 1)
    table[...] = jnp.zeros((16, square), jnp.float32)
    for c in range(comp):
        table[pl.ds(c, 1), pl.ds(0, n_x)] = scale_v[c]
    by_owner = jnp.transpose(jnp.concatenate([table[...], jnp.zeros((square - 16, square), jnp.float32)], axis=0))
    for owner in range(n_x):
        factor_send[owner] = by_owner[owner:owner + 1, :comp]
    inv_v[...] = jnp.full((1, square), -1, jnp.int32)
    inv_v[pl.ds(0, 1), pl.ds(0, n_x)] = perm_v[...]
    by_holder = jnp.transpose(jnp.broadcast_to(inv_v[...], (square, square)))
    inv_v[...] = jnp.max(jnp.where(by_holder == lane_q, sub_q, 0), axis=0, keepdims=True)
    inverse = pltpu.make_async_copy(inv_v, inv, loc_sem.at[0])
    inverse.start()
    own_factor = pltpu.make_async_copy(factor_send.at[me_x], factors.at[me_x], loc_sem.at[1])
    own_factor.start()

    def send_factors():
        for distance in near + far:
            factor_copy(distance).start()

    for step in range(STEPS):
        if step > 0:
            partials(step)
            send_stress_y(step)
            send_corners(step)
            x_start(step, DOWN_S, UP_S, DOWN_V, UP_V)
        if step == 1:
            pass
            words_of(beside, (1, far))
        velocity(step, inner, 0, (VX,))
        velocity(step, inner, last, (VY, VZ))
        over(1, last, functools.partial(velocity, step, inner))
        receive_y(step, STRESS_Y)
        velocity(step, outer, 0, (VX,))
        velocity(step, outer, last, (VY, VZ))
        over(1, last, functools.partial(velocity, step, outer))
        send_speed_y(step)
        if step == 0:
            send_factors()
            pass
            words_of(quick, (0, far))
        else:
            pass_relays()
            words_of(jnp.logical_not(beside), (1, far))
            send_words(1, near)
        over(1, last, functools.partial(stress, step, inner))
        if step == 1:
            own_factor.wait()
            for distance in near + far:
                factor_copy(distance).wait()
            to_scalar = pltpu.make_async_copy(factors, factor_s, loc_sem.at[1])
            to_scalar.start()
        x_wait(step, "recv", DOWN_S, DOWN_V, UP_S, UP_V)
        if step == 0:
            receive_y(STEPS, BUOY_Y)
            x_wait(0, "recv", DOWN_B, UP_B)
        receive_corners(step)
        complete(step)
        receive_y(step, SPEED_Y)
        if step == 0:
            pass
            pass
        fix_rows(step)
        ends(functools.partial(stress, step, every))
        over(1, last, functools.partial(stress, step, outer))
    to_scalar.wait()
    inverse.wait()
    receive_words(0)
    over(0, cx, functools.partial(gradient, 0))
    receive_words(STEPS - 1)
    over(0, cx, functools.partial(gradient, STEPS - 1))

    finish_relays()
    for step in range(STEPS):
        x_wait(step, "send", DOWN_S, DOWN_V, UP_S, UP_V)
        for message in STRESS_Y + SPEED_Y:
            @pl.when(edge(message[2], "gy"))
            def _():
                y_copy(step, message).wait_send()
        for which, (way_x, way_y, _, _) in enumerate(CORNERS):
            @pl.when(both_edges(way_x, way_y))
            def _():
                corner_copy(step, which).wait_send()
    for message in BUOY_Y:
        @pl.when(edge(message[2], "gy"))
        def _():
            y_copy(STEPS, message).wait_send()
    x_wait(0, "send", DOWN_B, UP_B)


def on_device(n_x, n_y, adjoint, buoyancy, lame_lambda, shear_mu, packed, scales, perm):
    fields, cx, cy, cz = adjoint.shape
    comp, segw = packed.shape[3:]
    lanes = min(128, segw)
    packed = packed.reshape(n_x, comp, segw // lanes, lanes)
    scales = jnp.transpose(scales, (0, 3, 2, 1)).reshape(comp, 1, n_x)
    halos = Y_SLOTS * STEPS + 2
    dma = pltpu.SemaphoreType.DMA
    f32, i32 = jnp.float32, jnp.int32
    return pl.pallas_call(
        functools.partial(kernel, n_x, n_y),
        out_shape=(pltpu.VMEM(adjoint.shape, f32), pltpu.VMEM((2, cx, cy, cz), f32)),
        in_specs=[pl.BlockSpec(memory_space=pltpu.HBM)] * 7,
        out_specs=(pl.BlockSpec(memory_space=pltpu.VMEM),) * 2,
        scratch_shapes=[
            pltpu.VMEM((fields, cx + 2, cy, cz), f32),
            pltpu.VMEM((3, cx, cy, cz), f32),
            pltpu.VMEM((comp, cx, cy, cz), f32),
            pltpu.VMEM((STEPS, 6, cy, cz), f32),
            pltpu.VMEM((2, cy, cz), f32),
            pltpu.VMEM((STEPS, 3, cy, cz), f32),
            pltpu.VMEM((STEPS, 5, 1, cz), f32),
            pltpu.VMEM((STEPS, 5, 1, cz), f32),
            pltpu.VMEM((halos, cx, cz), f32),
            pltpu.VMEM((halos, cx, cz), f32),
            pltpu.VMEM((max(32, 1), comp // STEPS, segw // lanes, lanes), i32),
            pltpu.VMEM((16, 128), f32),
            pltpu.VMEM((comp, 1, n_x), f32),
            pltpu.VMEM((n_x, 1, comp), f32),
            pltpu.VMEM((n_x, 1, comp), f32),
            pltpu.SMEM((n_x, 1, comp), f32),
            pltpu.VMEM((1, n_x), i32),
            pltpu.VMEM((1, 128), i32),
            pltpu.SMEM((1, 128), i32),
            dma((12,)), dma((STEPS, 6)), dma((STEPS, 6)), dma((STEPS, 4)), dma((STEPS, 4)), dma((max(32, 1),)), dma((max(32, 1),)), dma((halos,)), dma((halos,)),
            dma((n_x, STEPS)), dma((n_x, STEPS)), dma((n_x,)), dma((n_x,)), dma((2 + STEPS,)),
        ] + [pltpu.VMEM((n_x, comp // STEPS, segw // lanes, lanes), i32)] * STEPS,
        compiler_params=pltpu.CompilerParams(collective_id=0, has_side_effects=True,
                                             vmem_limit_bytes=64000000),
    )(adjoint, buoyancy, lame_lambda, shear_mu, packed, scales, perm)


def solution(mesh):
    return jax.shard_map(
        functools.partial(on_device, mesh.shape["gx"], mesh.shape["gy"]),
        mesh=mesh,
        in_specs=(
            P(None, "gx", "gy", None),
            P("gx", "gy", None),
            P("gx", "gy", None),
            P("gx", "gy", None),
            P("gx", None, "gy", None, None),
            P("gx", None, "gy", None),
            P("gx", None),
        ),
        out_specs=(P(None, "gx", "gy", None), P(None, "gx", "gy", None)),
        check_vma=False,
    )
```
